256 devices in a mesh: vis: 32 (over x, z), tile: 8 (over y, core).
Axes of the slice: x: 4, y: 4, z: 8, core: 2. Of those that a mesh axis runs over, the one named last changes fastest.
Arguments:
- spectra: bfloat16 [64, 2048], P(None, ('vis', 'tile')), may hold values from -0.1875 to 0.1875
- positions: int32 [2, 2048], P(None, ('vis', 'tile')), may hold values from 0 to 8191
- observed: bfloat16 [262144, 128], P(('vis', 'tile')), may hold values from -6 to 6
- cells: int32 [2, 262144], P(None, ('vis', 'tile')), may hold values from 0 to 8184, as said below
- fractions: float32 [2, 262144], P(None, ('vis', 'tile')), may hold values from 0 to 1
- bucket_counts: int32 [256, 8], P(('vis', 'tile')), may hold values from 0 to 512, as said below
- chan_weights: float32 [64], replicated, may hold values from 0.04 to 0.32
Outputs:
- residual_vis: bfloat16 [262144, 128], P(('vis', 'tile'))
- residual_grid: float32 [128, 2, 8192], P('vis', None, 'tile')
The draws below stay inside these ranges and needn't reach their ends.
Inputs may be any that keep to these rules, and one draw needn't show every extreme that they name: cells[0, r] is the first uv column and cells[1, r] the first uv row of row r's 8 x 8 kernel window, with cells[1, r] <= 120. The rows of each device are ordered by tile: for device d and tile t, the bucket_counts[d, t] rows that start after the first sum of bucket_counts[d, 0:t] rows have cells[0] between t * 1024 and (t + 1) * 1024 - 8; rows after a device's total are unused. `bucket_counts`: each device's counts sum to at most 1024. For every index of vis, one tile receives exactly 512 rows from every device with that vis index; which tile is drawn.
All inputs are finite; a program needn't handle non-finite values.
Results may differ from the reference program's by a relative error of at most 0.008.
Values may be sent and summed in bfloat16 or wider, within the bound.
No kernel may reach another device: no remote copies, remote signals or barrier semaphores. Data moves between devices by JAX's collectives and lax.ppermute only.
A program may use at most 64 MiB of HBM per device.

```python
import math
import jax
import jax.numpy as jnp
from jax import lax

COMPS = 2048
CHANS = 64
GRID = 8192
BAND = 128
ROWS_DEV = 1024
TAPS = 8
SLOT = 512
TILE_W = 1024
ROWS = 262144
N_VIS = 32
N_TILE = 8


def bucket_layout(key):
    folded = jax.random.fold_in(key, 7)
    device_total = N_VIS * N_TILE
    hottest = jax.random.randint(jax.random.fold_in(folded, 1), (N_VIS,), 0, N_TILE)
    others_most = (ROWS_DEV - SLOT) // (N_TILE - 1)
    others = jax.random.randint(jax.random.fold_in(folded, 2), (N_VIS, N_TILE, N_TILE), others_most // 4, others_most + 1)
    is_hottest = jnp.arange(N_TILE)[None, None, :] == hottest[:, None, None]
    return jnp.where(is_hottest, SLOT, others).reshape(device_total, N_TILE).astype(jnp.int32)


def draw_bucket_counts(key, part):
    return bucket_layout(key)


def draw_cells(key, part):
    folded = jax.random.fold_in(key, 7)
    device_total = N_VIS * N_TILE
    bucket_sizes = bucket_layout(key)
    bucket_ends = jnp.cumsum(bucket_sizes, axis=1)
    local_index = jnp.arange(ROWS_DEV, dtype=jnp.int32)
    tile_of = jnp.sum((local_index[None, :, None] >= bucket_ends[:, None, :]).astype(jnp.int32), axis=2)
    spare_tile = jax.random.randint(jax.random.fold_in(folded, 3), (device_total, ROWS_DEV), 0, N_TILE)
    tile_of = jnp.where(tile_of >= N_TILE, spare_tile, tile_of)
    within = jax.random.randint(jax.random.fold_in(folded, 4), (device_total, ROWS_DEV), 0, TILE_W - TAPS + 1)
    first_col = tile_of * TILE_W + within
    first_row = jax.random.randint(jax.random.fold_in(folded, 5), (device_total, ROWS_DEV), 0, BAND - TAPS + 1)
    return jnp.stack([first_col.reshape(-1), first_row.reshape(-1)]).astype(jnp.int32)


def plant(drawn, stream_key, smallest, top_value):
    longest = drawn.shape.index(max(drawn.shape))
    spots = []
    for shift in (0, 1):
        where = [jax.random.randint(jax.random.fold_in(stream_key, axis), (), 0, length) for axis, length in enumerate(drawn.shape)]
        where[longest] = (where[longest] + shift) % drawn.shape[longest]
        spots.append(tuple(where))
    return drawn.at[spots[0]].set(smallest).at[spots[1]].set(top_value)


def block_levels(key, shape, cuts, least, high):
    def one(dim, blocks):
        heights = jax.random.uniform(jax.random.fold_in(jax.random.fold_in(key, 6), dim), (blocks,), jnp.float32, least / len(cuts), high / len(cuts))
        return jnp.repeat(jnp.exp(heights), shape[dim] // blocks).reshape((-1,) + (1,) * (len(shape) - dim - 1))

    level = one(*cuts[0])
    for cut in cuts[1:]:
        level = level * one(*cut)
    return level


def normal_values(stream_key, extent, deviation, limit, pieces=(), kind=jnp.bfloat16):
    drawn = jax.random.normal(stream_key, extent, jnp.float32) * deviation
    if len(pieces) > 0:
        drawn = block_levels(stream_key, extent, pieces, -0.22, 0.18) * drawn
    return jnp.clip(drawn, min=-limit, max=limit).astype(kind)


def setup_inputs(seed: int = 0) -> dict:
    streams_of = jax.random.split(jax.random.key(seed), 8)
    return {
        "spectra": normal_values(streams_of[0], (CHANS, COMPS), (COMPS // 2) ** -0.5, 0.1875, ((1, 256),)),
        "positions": plant(jax.random.randint(streams_of[1], (2, COMPS), 0, GRID), jax.random.fold_in(streams_of[1], 1), 0, GRID - 1).astype(jnp.int32),
        "observed": normal_values(streams_of[2], (ROWS, 2 * CHANS), 1.0, 6.0, ((0, 256),)),
        "cells": draw_cells(jax.random.fold_in(streams_of[7], 71), 0),
        "fractions": jnp.clip(1.0 * jax.random.uniform(streams_of[4], (2, ROWS), jnp.float32) ** block_levels(streams_of[4], (2, ROWS), ((1, 256),), -0.2, 0.2), 0.0, 1.0),
        "bucket_counts": draw_bucket_counts(jax.random.fold_in(streams_of[7], 71), 0),
        "chan_weights": jnp.clip(jnp.exp(jax.random.uniform(streams_of[6], (CHANS,), jnp.float32, math.log(0.04), math.log(0.32))), 0.04, 0.32),
    }


def kernel_taps(offsets):
    taps_float = jnp.arange(TAPS, dtype=jnp.int32).astype(jnp.float32)
    shifted = (taps_float[None, :] - 3.0) - offsets[:, None]
    return jnp.exp(-0.5 * (shifted * shifted))


def reference(spectra, positions, observed, cells, fractions, bucket_counts, chan_weights):
    row_total = observed.shape[0]
    col_pixel = positions[0]
    row_pixel = positions[1]
    spectra_cols = spectra.T

    def predict_block(block_data):
        first_col, first_row, col_frac, row_frac = block_data
        turn_count = jnp.mod((first_col + 3)[:, None] * col_pixel[None, :] + (first_row + 3)[:, None] * row_pixel[None, :], GRID)
        phase_turns = turn_count.astype(jnp.float32) + col_frac[:, None] * col_pixel.astype(jnp.float32)[None, :] + row_frac[:, None] * row_pixel.astype(jnp.float32)[None, :]
        angles = phase_turns * (2.0 * math.pi / GRID)
        cosine = jnp.cos(angles).astype(jnp.bfloat16)
        sine_table = jnp.sin(angles).astype(jnp.bfloat16)
        real_part = jnp.dot(cosine, spectra_cols, preferred_element_type=jnp.float32)
        imag_part = -jnp.dot(sine_table, spectra_cols, preferred_element_type=jnp.float32)
        return jnp.concatenate([real_part, imag_part], axis=1)

    block_count = row_total // ROWS_DEV
    shaped = lambda array: array.reshape(block_count, ROWS_DEV)
    predicted = lax.map(predict_block, (shaped(cells[0]), shaped(cells[1]), shaped(fractions[0]), shaped(fractions[1])))
    predicted = predicted.reshape(row_total, 2 * CHANS)

    live_rows = jnp.sum(bucket_counts, axis=1)
    local_index = jnp.arange(ROWS_DEV, dtype=jnp.int32)
    row_live = (local_index[None, :] < live_rows[:, None]).reshape(row_total)
    residual = jnp.where(row_live[:, None], observed.astype(jnp.float32) - predicted, 0.0).astype(jnp.bfloat16)
    widened = residual.astype(jnp.float32)
    value_real = jnp.sum(widened[:, :CHANS] * chan_weights[None, :], axis=1)
    value_imag = jnp.sum(widened[:, CHANS:] * chan_weights[None, :], axis=1)

    row_kernel = kernel_taps(fractions[1])
    col_kernel = lax.optimization_barrier(kernel_taps(fractions[0]).astype(jnp.bfloat16)).astype(jnp.float32)
    left_real = lax.optimization_barrier((value_real[:, None] * row_kernel).astype(jnp.bfloat16)).astype(jnp.float32)
    left_imag = lax.optimization_barrier((value_imag[:, None] * row_kernel).astype(jnp.bfloat16)).astype(jnp.float32)

    taps_index = jnp.arange(TAPS, dtype=jnp.int32)
    row_index = jnp.broadcast_to(cells[1][:, None, None] + taps_index[None, :, None], (row_total, TAPS, TAPS))
    col_index = jnp.broadcast_to(cells[0][:, None, None] + taps_index[None, None, :], (row_total, TAPS, TAPS))
    contrib_real = left_real[:, :, None] * col_kernel[:, None, :]
    contrib_imag = left_imag[:, :, None] * col_kernel[:, None, :]
    grid_sum = jnp.zeros((BAND, 2, GRID), jnp.float32)
    grid_sum = grid_sum.at[row_index, 0, col_index].add(contrib_real)
    grid_sum = grid_sum.at[row_index, 1, col_index].add(contrib_imag)
    return residual, grid_sum
```

```python
import jax
import jax.numpy as jnp
from jax import lax
from jax.experimental import pallas as pl
from jax.experimental.pallas import tpu as pltpu
from jax.sharding import Mesh
from jax.sharding import PartitionSpec as P

GRID = 8192
BAND = 128
TAPS = 8
TILE = ("tile_0", "tile_1")
VIS = ("vis_0", "vis_1")
VIS_TILE = ("vis_0", "vis_1", "tile_0", "tile_1")
DIGIT_LANE = 64
F32 = jnp.float32
BF16 = jnp.bfloat16
NT = (((1,), (1,)), ((), ()))
NN = (((1,), (0,)), ((), ()))

COS_POLY = (1.4142135, -6.97885099, 5.73946112, -1.88356261, 0.31069733)
SIN_POLY = (4.4428679, -7.30744333, 3.59478717, -0.78437159)
ROUND = 12582912.0


def three_parts(value):
    first = value.astype(BF16).astype(F32)
    rest = value - first
    second = rest.astype(BF16).astype(F32)
    return [first, second, rest - second]


def component_rows(spectra, positions):
    low = ((positions + 64) & 127) - 64
    high = (positions - low) >> 7
    digits = jnp.concatenate(
        [
            jnp.broadcast_to(d[None], (n, d.shape[0]))
            for d, n in ((high[0], 4), (low[0], 5), (high[1], 4), (low[1], 5))
        ]
    ).astype(BF16)
    rows = jnp.concatenate([spectra, digits])
    return jnp.pad(rows, ((0, 128 - rows.shape[0]), (0, 0))).T


def row_factors(cells, fractions):
    parts = []
    for axis in range(2):
        first = cells[axis : axis + 1] + 3
        low = ((first + 32) & 63) - 32
        high = first - low
        frac = three_parts(fractions[axis : axis + 1])
        parts += [low.astype(F32) * (128.0 / GRID)] + [f * (128.0 / GRID) for f in frac]
        high = ((high + GRID // 2) & (GRID - 1)) - GRID // 2
        parts += [high.astype(F32) * (1.0 / GRID), low.astype(F32) * (1.0 / GRID)]
        parts += [f * (1.0 / GRID) for f in frac]
    return parts


def polynomial(coefficients, s):
    result = coefficients[-1] * s + coefficients[-2]
    for c in coefficients[-3::-1]:
        result = result * s + c
    return result


def predict_kernel(counts, comps, cells, fractions, observed, weights, residual, packed, factors, fields):
    rows = observed.shape[0]
    slot = packed.shape[2]
    tiles = packed.shape[0]
    comp_total = comps.shape[0]
    parts = row_factors(cells[...], fractions[...])
    lead = jnp.zeros((DIGIT_LANE, rows), F32)
    tail = jnp.zeros((128 - DIGIT_LANE - len(parts), rows), F32)
    factors[...] = jnp.concatenate([lead] + parts + [tail]).T.astype(BF16)

    start = []
    total = counts[0, 0] * 0
    for t in range(tiles):
        start.append(total)
        total = total + counts[0, t]

    w = weights[...]
    both = jnp.concatenate([w, w], axis=1)
    lane = lax.broadcasted_iota(jnp.int32, both.shape, 1)
    w_re = three_parts(jnp.where(lane < 64, both, 0.0))
    w_im = three_parts(jnp.where(lane < 64, 0.0, both))
    w_rows = jnp.concatenate(w_re + w_im + [jnp.zeros((2, 128), F32)]).astype(BF16)

    block = 256
    comp_block = 256

    def row_step(step, carry):
        at = pl.ds(step * block, block)
        left = factors[at, :]
        acc_cos = jnp.zeros((block, 128), F32)
        acc_sin = jnp.zeros((block, 128), F32)
        for k in range(comp_total // comp_block):
            piece = comps[k * comp_block : (k + 1) * comp_block, :]
            turns = lax.dot_general(left, piece, NT, preferred_element_type=F32)
            y = turns - ((turns + ROUND) - ROUND)
            s = y * y
            c = polynomial(COS_POLY, s)
            d = polynomial(SIN_POLY, s) * y
            cosine = (1.0 - d * d).astype(BF16)
            sine = (c * d).astype(BF16)
            acc_cos += lax.dot_general(cosine, piece, NN, preferred_element_type=F32)
            acc_sin += lax.dot_general(sine, piece, NN, preferred_element_type=F32)
        lanes = lax.broadcasted_iota(jnp.int32, (block, 128), 1)
        index = lax.broadcasted_iota(jnp.int32, (block, 128), 0) + step * block
        predicted = jnp.where(lanes < 64, acc_cos, -pltpu.roll(acc_sin, 64, 1))
        res = jnp.where(index < total, observed[at, :].astype(F32) - predicted, 0.0).astype(BF16)
        residual[at, :] = res
        sums = lax.dot_general(w_rows, res, NT, preferred_element_type=F32)
        fields[0:1, at] = sums[0:1] + sums[1:2] + sums[2:3]
        fields[1:2, at] = sums[3:4] + sums[4:5] + sums[5:6]
        return carry

    lax.fori_loop(0, rows // block, row_step, 0)
    fields[2:4, :] = fractions[...]
    fields[4:6, :] = cells[...].astype(F32)
    fields[6:8, :] = jnp.zeros((2, rows), F32)
    everything = fields[...]
    row_of = lax.broadcasted_iota(jnp.int32, (8, slot), 0)
    place = lax.broadcasted_iota(jnp.int32, (8, slot), 1)
    for t in range(tiles):
        moved = pltpu.roll(everything, (rows - start[t]) & (rows - 1), 1)[:, :slot]
        moved = jnp.where((row_of >= 2) | (place < counts[0, t]), moved, 0.0)
        base = float(t * (GRID // tiles))
        packed[t] = moved - jnp.where(row_of == 4, base, 0.0)


def grid_kernel(got, out, acc):
    sources, _, slot = got.shape
    width = acc.shape[1]
    high = acc.shape[0]
    scale = -0.7213475204444817
    acc[...] = jnp.zeros(acc.shape, F32)
    line = lax.broadcasted_iota(jnp.int32, (high, slot), 0)
    line_row = line >> 1
    imag = (line & 1) == 1

    def source_step(step, carry):
        data = got[step]
        first_row = data[5:6, :].astype(jnp.int32)
        value = jnp.where(imag, data[1:2, :], data[0:1, :])
        tap = line_row - first_row
        off = (tap - 3).astype(F32) - data[3:4, :]
        kernel = jnp.exp2(off * off * scale)
        left = jnp.where((tap & ~7) == 0, value * kernel, 0.0).astype(BF16)
        turned = data.T
        block = 128
        cols = []
        for r in range(slot // block):
            sub = turned[r * block : (r + 1) * block]
            first_col = sub[:, 4:5].astype(jnp.int32)
            col_frac = sub[:, 2:3]
            column = lax.broadcasted_iota(jnp.int32, (block, width), 1)
            tap_u = column - first_col
            off_u = (tap_u - 3).astype(F32) - col_frac
            weight = jnp.exp2(off_u * off_u * scale)
            cols.append(jnp.where((tap_u & ~7) == 0, weight, 0.0).astype(BF16))
        spread = jnp.concatenate(cols)
        acc[...] += lax.dot_general(left, spread, NN, preferred_element_type=F32)
        return carry

    lax.fori_loop(0, sources, source_step, 0)
    out[...] = acc[...].astype(BF16).reshape(out.shape)


def on_device(spectra, positions, observed, cells, fractions, bucket_counts, chan_weights):
    rows = observed.shape[0]
    tiles = lax.axis_size(TILE)
    owners = lax.axis_size(VIS)
    slot = rows // 2
    width = GRID // tiles
    devices = tiles * owners
    mine = component_rows(spectra, positions)
    comps = lax.all_to_all(
        jnp.broadcast_to(mine[None], (devices,) + mine.shape), VIS_TILE, 0, 0, tiled=True
    ).reshape(devices * mine.shape[0], 128)
    vmem = pl.BlockSpec(memory_space=pltpu.VMEM)
    residual, packed = pl.pallas_call(
        predict_kernel,
        out_shape=(
            jax.ShapeDtypeStruct(observed.shape, BF16),
            jax.ShapeDtypeStruct((tiles, 8, slot), F32),
        ),
        in_specs=[pl.BlockSpec(memory_space=pltpu.SMEM)] + [vmem] * 5,
        out_specs=(vmem, vmem),
        scratch_shapes=[pltpu.VMEM((rows, 128), BF16), pltpu.VMEM((8, rows), F32)],
        name="predict",
    )(bucket_counts, comps, cells, fractions, observed, chan_weights[None, :])
    got = lax.all_to_all(packed, TILE, 0, 0, tiled=True)
    share = BAND // owners
    partial = pl.pallas_call(
        grid_kernel,
        out_shape=jax.ShapeDtypeStruct((owners, 2 * share, width), BF16),
        in_specs=[vmem],
        out_specs=vmem,
        scratch_shapes=[pltpu.VMEM((2 * BAND, width), F32)],
        name="gridding",
    )(got)
    parts = lax.all_to_all(partial, VIS, 0, 0, tiled=True)
    total = jnp.sum(parts.astype(F32), axis=0)
    return residual, total.reshape(share, 2, width)


def solution(mesh):
    torus = Mesh(mesh.devices.reshape(4, 8, 4, 2), ("vis_0", "vis_1", "tile_0", "tile_1"))
    return jax.shard_map(
        on_device,
        mesh=torus,
        in_specs=(
            P(None, VIS_TILE),
            P(None, VIS_TILE),
            P(VIS_TILE, None),
            P(None, VIS_TILE),
            P(None, VIS_TILE),
            P(VIS_TILE, None),
            P(),
        ),
        out_specs=(P(VIS_TILE, None), P(VIS, None, TILE)),
        check_vma=False,
    )
```

```python
import jax
import jax.numpy as jnp
from jax import lax
from jax.experimental import pallas as pl
from jax.experimental.pallas import tpu as pltpu
from jax.sharding import Mesh
from jax.sharding import PartitionSpec as P

GRID = 8192
BAND = 128
TAPS = 8
TILE = ("tile_0", "tile_1")
VIS = ("vis_0", "vis_1")
VIS_TILE = ("vis_0", "vis_1", "tile_0", "tile_1")
DIGIT_LANE = 64
F32 = jnp.float32
BF16 = jnp.bfloat16
NT = (((1,), (1,)), ((), ()))
NN = (((1,), (0,)), ((), ()))

COS_POLY = (1.41420408, -6.97764191, 5.71523647, -1.72834251)
SIN_POLY = (4.4428679, -7.30744333, 3.59478717, -0.78437159)
ROUND = 12582912.0


def three_parts(value):
    first = value.astype(BF16).astype(F32)
    rest = value - first
    second = rest.astype(BF16).astype(F32)
    return [first, second, rest - second]


def component_rows(spectra, positions):
    low = ((positions + 64) & 127) - 64
    high = (positions - low) >> 7
    digits = jnp.concatenate(
        [
            jnp.broadcast_to(d[None], (n, d.shape[0]))
            for d, n in ((high[0], 4), (low[0], 5), (high[1], 4), (low[1], 5))
        ]
    ).astype(BF16)
    rows = jnp.concatenate([spectra, digits])
    return jnp.pad(rows, ((0, 128 - rows.shape[0]), (0, 0))).T


def row_factors(cells, fractions):
    parts = []
    for axis in range(2):
        first = cells[axis : axis + 1] + 3
        low = ((first + 32) & 63) - 32
        high = first - low
        frac = three_parts(fractions[axis : axis + 1])
        parts += [low.astype(F32) * (128.0 / GRID)] + [f * (128.0 / GRID) for f in frac]
        high = ((high + GRID // 2) & (GRID - 1)) - GRID // 2
        parts += [high.astype(F32) * (1.0 / GRID), low.astype(F32) * (1.0 / GRID)]
        parts += [f * (1.0 / GRID) for f in frac]
    return parts


def monic(coefficients, s):
    lead = coefficients[-1]
    result = s + coefficients[-2] / lead
    for c in coefficients[-3::-1]:
        result = result * s + c / lead
    return result


def polynomial(coefficients, s):
    result = coefficients[-1] * s + coefficients[-2]
    for c in coefficients[-3::-1]:
        result = result * s + c
    return result


def predict_kernel(counts, here, there, cells, fractions, observed, weights, residual, packed, factors, fields):
    rows = observed.shape[0]
    slot = packed.shape[2]
    tiles = packed.shape[0]
    comp_total = here.shape[0]
    parts = row_factors(cells[...], fractions[...])
    lead = jnp.zeros((DIGIT_LANE, rows), F32)
    tail = jnp.zeros((128 - DIGIT_LANE - len(parts), rows), F32)
    factors[...] = jnp.concatenate([lead] + parts + [tail]).T.astype(BF16)

    start = []
    total = counts[0, 0] * 0
    for t in range(tiles):
        start.append(total)
        total = total + counts[0, t]

    w = weights[...]
    both = jnp.concatenate([w, w], axis=1)
    lane = lax.broadcasted_iota(jnp.int32, both.shape, 1)
    w_re = three_parts(jnp.where(lane < 64, both, 0.0))
    w_im = three_parts(jnp.where(lane < 64, 0.0, both))
    w_rows = jnp.concatenate(w_re + w_im + [jnp.zeros((2, 128), F32)]).astype(BF16)

    block = 1024
    comp_block = 256

    def row_step(step, carry):
        at = pl.ds(step * block, block)
        left = factors[at, :]
        acc_cos = jnp.zeros((block, 128), F32)
        acc_sin = jnp.zeros((block, 128), F32)
        for k in range(2 * comp_total // comp_block):
            comps = here if k * comp_block < comp_total else there
            piece_at = k * comp_block % comp_total
            piece = comps[piece_at : piece_at + comp_block, :]
            turns = lax.dot_general(left, piece, NT, preferred_element_type=F32)
            y = turns - ((turns + ROUND) - ROUND)
            s = y * y
            c = monic(COS_POLY, s)
            d = monic(SIN_POLY, s) * y
            cosine = (1.0 / SIN_POLY[-1] ** 2 - d * d).astype(BF16)
            sine = (c * d).astype(BF16)
            acc_cos += lax.dot_general(cosine, piece, NN, preferred_element_type=F32)
            acc_sin += lax.dot_general(sine, piece, NN, preferred_element_type=F32)
        lanes = lax.broadcasted_iota(jnp.int32, (block, 128), 1)
        index = lax.broadcasted_iota(jnp.int32, (block, 128), 0) + step * block
        predicted = jnp.where(lanes < 64, acc_cos * SIN_POLY[-1] ** 2, pltpu.roll(acc_sin, 64, 1) * (-COS_POLY[-1] * SIN_POLY[-1]))
        res = jnp.where(index < total, observed[at, :].astype(F32) - predicted, 0.0).astype(BF16)
        residual[at, :] = res
        sums = lax.dot_general(w_rows, res, NT, preferred_element_type=F32)
        fields[0:1, at] = sums[0:1] + sums[1:2] + sums[2:3]
        fields[1:2, at] = sums[3:4] + sums[4:5] + sums[5:6]
        return carry

    lax.fori_loop(0, rows // block, row_step, 0)
    fields[2:4, :] = fractions[...]
    fields[4:6, :] = cells[...].astype(F32)
    fields[6:8, :] = jnp.zeros((2, rows), F32)
    everything = fields[...]
    row_of = lax.broadcasted_iota(jnp.int32, (8, slot), 0)
    place = lax.broadcasted_iota(jnp.int32, (8, slot), 1)
    for t in range(tiles):
        moved = pltpu.roll(everything, (rows - start[t]) & (rows - 1), 1)[:, :slot]
        moved = jnp.where((row_of >= 2) | (place < counts[0, t]), moved, 0.0)
        base = float(t * (GRID // tiles))
        packed[t] = moved - jnp.where(row_of == 4, base, 0.0)


def grid_kernel(got, out, acc):
    sources, _, slot = got.shape
    slot = slot * 4
    sources = sources // 4
    width = acc.shape[1]
    high = acc.shape[0]
    scale = -0.7213475204444817
    acc[...] = jnp.zeros(acc.shape, F32)
    line = lax.broadcasted_iota(jnp.int32, (high, slot), 0)
    line_row = line >> 1
    line_float = line_row.astype(F32)
    imag = (line & 1) == 1
    block = 128
    column = lax.broadcasted_iota(jnp.int32, (block, width), 1)
    column_float = column.astype(F32)

    def source_step(step, carry):
        data = jnp.concatenate([got[step * 4 + k] for k in range(4)], axis=1)
        value = jnp.where(imag, data[1:2, :], data[0:1, :])
        off = line_float - (data[5:6, :] + 3.0 + data[3:4, :])
        kernel = jnp.exp2(off * off * scale)
        near = (lambda t: t.astype(jnp.uint32) < 8)(line_row - data[5:6, :].astype(jnp.int32))
        left = jnp.where(near, value * kernel, 0.0).astype(BF16)
        turned = jnp.concatenate([data[4:5], data[4:5] + 3.0 + data[2:3], data[:6]]).T
        cols = []
        for r in range(slot // block):
            sub = turned[r * block : (r + 1) * block]
            first_col = sub[:, 0:1].astype(jnp.int32)
            off_u = column_float - sub[:, 1:2]
            weight = jnp.exp2(off_u * off_u * scale)
            cols.append(jnp.where((lambda t: t.astype(jnp.uint32) < 8)(column - first_col), weight, 0.0).astype(BF16))
        spread = jnp.concatenate(cols)
        acc[...] += lax.dot_general(left, spread, NN, preferred_element_type=F32)
        return carry

    lax.fori_loop(0, sources, source_step, 0)
    out[...] = acc[...].astype(BF16).reshape(out.shape)


def on_device(spectra, positions, observed, cells, fractions, bucket_counts, chan_weights):
    rows = observed.shape[0]
    tiles = lax.axis_size(TILE)
    owners = lax.axis_size(VIS)
    slot = rows // 2
    width = GRID // tiles
    devices = tiles * owners
    mine = component_rows(spectra, positions)
    same_core = VIS + ("tile_0",)
    half = devices // lax.axis_size("tile_1")
    here = lax.all_to_all(
        jnp.broadcast_to(mine[None], (half,) + mine.shape), same_core, 0, 0, tiled=True
    ).reshape(half * mine.shape[0], 128)
    there = lax.ppermute(here, "tile_1", [(0, 1), (1, 0)])
    vmem = pl.BlockSpec(memory_space=pltpu.VMEM)
    residual, packed = pl.pallas_call(
        predict_kernel,
        out_shape=(
            jax.ShapeDtypeStruct(observed.shape, BF16),
            jax.ShapeDtypeStruct((tiles, 8, slot), F32),
        ),
        in_specs=[pl.BlockSpec(memory_space=pltpu.SMEM)] + [vmem] * 6,
        out_specs=(vmem, vmem),
        scratch_shapes=[pltpu.VMEM((rows, 128), BF16), pltpu.VMEM((8, rows), F32)],
        name="predict",
    )(bucket_counts, here, there, cells, fractions, observed, chan_weights[None, :])
    got = lax.all_to_all(packed, TILE, 0, 0, tiled=True)
    share = BAND // owners
    partial = pl.pallas_call(
        grid_kernel,
        out_shape=jax.ShapeDtypeStruct((owners, 2 * share, width), BF16),
        in_specs=[vmem],
        out_specs=vmem,
        scratch_shapes=[pltpu.VMEM((2 * BAND, width), F32)],
        name="gridding",
    )(got)
    parts = lax.all_to_all(partial, VIS, 0, 0, tiled=True)
    total = jnp.sum(parts.astype(F32), axis=0)
    return residual, total.reshape(share, 2, width)


def solution(mesh):
    torus = Mesh(mesh.devices.reshape(4, 8, 4, 2), ("vis_0", "vis_1", "tile_0", "tile_1"))
    return jax.shard_map(
        on_device,
        mesh=torus,
        in_specs=(
            P(None, VIS_TILE),
            P(None, VIS_TILE),
            P(VIS_TILE, None),
            P(None, VIS_TILE),
            P(None, VIS_TILE),
            P(VIS_TILE, None),
            P(),
        ),
        out_specs=(P(VIS_TILE, None), P(VIS, None, TILE)),
        check_vma=False,
    )
```

```python
import jax
import jax.numpy as jnp
from jax import lax
from jax.experimental import pallas as pl
from jax.experimental.pallas import tpu as pltpu
from jax.sharding import Mesh
from jax.sharding import PartitionSpec as P

GRID = 8192
BAND = 128
TAPS = 8
TILE = ("tile_0", "tile_1")
VIS = ("vis_0", "vis_1")
VIS_TILE = ("vis_0", "vis_1", "tile_0", "tile_1")
DIGIT_LANE = 64
F32 = jnp.float32
BF16 = jnp.bfloat16
NT = (((1,), (1,)), ((), ()))
NN = (((1,), (0,)), ((), ()))

COS_POLY = (1.41420408, -6.97764191, 5.71523647, -1.72834251)
SIN_POLY = (4.4428679, -7.30744333, 3.59478717, -0.78437159)
LIMIT = pltpu.CompilerParams(vmem_limit_bytes=24 * 2**20)
ROUND = 12582912.0


def three_parts(value):
    first = value.astype(BF16).astype(F32)
    rest = value - first
    second = rest.astype(BF16).astype(F32)
    return [first, second, rest - second]


def component_rows(spectra, positions):
    low = ((positions + 64) & 127) - 64
    high = (positions - low) >> 7
    digits = jnp.concatenate(
        [
            jnp.broadcast_to(d[None], (n, d.shape[0]))
            for d, n in ((high[0], 4), (low[0], 5), (high[1], 4), (low[1], 5))
        ]
    ).astype(BF16)
    rows = jnp.concatenate([spectra, digits])
    return jnp.pad(rows, ((0, 128 - rows.shape[0]), (0, 0))).T


def row_factors(cells, fractions):
    parts = []
    for axis in range(2):
        first = cells[axis : axis + 1] + 3
        low = ((first + 32) & 63) - 32
        high = first - low
        frac = three_parts(fractions[axis : axis + 1])
        parts += [low.astype(F32) * (128.0 / GRID)] + [f * (128.0 / GRID) for f in frac]
        high = ((high + GRID // 2) & (GRID - 1)) - GRID // 2
        parts += [high.astype(F32) * (1.0 / GRID), low.astype(F32) * (1.0 / GRID)]
        parts += [f * (1.0 / GRID) for f in frac]
    return parts


def monic(coefficients, s):
    lead = coefficients[-1]
    result = s + coefficients[-2] / lead
    for c in coefficients[-3::-1]:
        result = result * s + c / lead
    return result


def polynomial(coefficients, s):
    result = coefficients[-1] * s + coefficients[-2]
    for c in coefficients[-3::-1]:
        result = result * s + c
    return result


def add_products(left, comps, cos_sum, sin_sum):
    comp_block = 256
    for first in range(0, comps.shape[0], comp_block):
        piece = comps[first : first + comp_block, :]
        turns = lax.dot_general(left, piece, NT, preferred_element_type=F32)
        y = turns - ((turns + ROUND) - ROUND)
        s = y * y
        c = monic(COS_POLY, s)
        d = monic(SIN_POLY, s) * y
        cosine = (1.0 / SIN_POLY[-1] ** 2 - d * d).astype(BF16)
        sine = (c * d).astype(BF16)
        cos_sum += lax.dot_general(cosine, piece, NN, preferred_element_type=F32)
        sin_sum += lax.dot_general(sine, piece, NN, preferred_element_type=F32)
    return cos_sum, sin_sum


def first_kernel(*refs):
    pieces, (cells, fractions, factors, cos_out, sin_out) = refs[:-5], refs[-5:]
    rows = factors.shape[0]
    parts = row_factors(cells[...], fractions[...])
    lead = jnp.zeros((DIGIT_LANE, rows), F32)
    tail = jnp.zeros((128 - DIGIT_LANE - len(parts), rows), F32)
    left = jnp.concatenate([lead] + parts + [tail]).T.astype(BF16)
    factors[...] = left
    cos_sum = jnp.zeros((rows, 128), F32)
    sin_sum = jnp.zeros((rows, 128), F32)
    for comps in pieces:
        cos_sum, sin_sum = add_products(left, comps, cos_sum, sin_sum)
    cos_out[...] = cos_sum
    sin_out[...] = sin_sum


def second_kernel(
    counts, comps, factors, cos_in, sin_in, cells, fractions, observed, weights, residual, packed, fields
):
    rows = observed.shape[0]
    slot = packed.shape[2]
    tiles = packed.shape[0]
    start = []
    total = counts[0, 0] * 0
    for t in range(tiles):
        start.append(total)
        total = total + counts[0, t]

    w = weights[...]
    both = jnp.concatenate([w, w], axis=1)
    lane = lax.broadcasted_iota(jnp.int32, both.shape, 1)
    w_re = three_parts(jnp.where(lane < 64, both, 0.0))
    w_im = three_parts(jnp.where(lane < 64, 0.0, both))
    w_rows = jnp.concatenate(w_re + w_im + [jnp.zeros((2, 128), F32)]).astype(BF16)

    cos_sum, sin_sum = add_products(factors[...], comps, cos_in[...], sin_in[...])
    lanes = lax.broadcasted_iota(jnp.int32, (rows, 128), 1)
    index = lax.broadcasted_iota(jnp.int32, (rows, 128), 0)
    real = cos_sum * SIN_POLY[-1] ** 2
    imag = pltpu.roll(sin_sum, 64, 1) * (-COS_POLY[-1] * SIN_POLY[-1])
    predicted = jnp.where(lanes < 64, real, imag)
    res = jnp.where(index < total, observed[...].astype(F32) - predicted, 0.0).astype(BF16)
    residual[...] = res
    sums = lax.dot_general(w_rows, res, NT, preferred_element_type=F32)
    fields[0:1, :] = sums[0:1] + sums[1:2] + sums[2:3]
    fields[1:2, :] = sums[3:4] + sums[4:5] + sums[5:6]
    fields[2:4, :] = fractions[...]
    fields[4:6, :] = cells[...].astype(F32)
    fields[6:8, :] = jnp.zeros((2, rows), F32)
    everything = fields[...]
    row_of = lax.broadcasted_iota(jnp.int32, (8, slot), 0)
    place = lax.broadcasted_iota(jnp.int32, (8, slot), 1)
    for t in range(tiles):
        moved = pltpu.roll(everything, (rows - start[t]) & (rows - 1), 1)[:, :slot]
        moved = jnp.where((row_of >= 2) | (place < counts[0, t]), moved, 0.0)
        base = float(t * (GRID // tiles))
        packed[t] = moved - jnp.where(row_of == 4, base, 0.0)


def grid_kernel(got, out, acc):
    sources, _, slot = got.shape
    slot = slot * 4
    sources = sources // 4
    width = acc.shape[1]
    high = acc.shape[0]
    scale = -0.7213475204444817
    acc[...] = jnp.zeros(acc.shape, F32)
    line = lax.broadcasted_iota(jnp.int32, (high, slot), 0)
    line_row = line >> 1
    line_float = line_row.astype(F32)
    imag = (line & 1) == 1
    block = 128
    column = lax.broadcasted_iota(jnp.int32, (block, width), 1)
    column_float = column.astype(F32)

    def source_step(step, carry):
        data = jnp.concatenate([got[step * 4 + k] for k in range(4)], axis=1)
        value = jnp.where(imag, data[1:2, :], data[0:1, :])
        off = line_float - (data[5:6, :] + 3.0 + data[3:4, :])
        kernel = jnp.exp2(off * off * scale)
        near = (lambda t: t.astype(jnp.uint32) < 8)(line_row - data[5:6, :].astype(jnp.int32))
        left = jnp.where(near, value * kernel, 0.0).astype(BF16)
        turned = jnp.concatenate([data[4:5], data[4:5] + 3.0 + data[2:3], data[:6]]).T
        cols = []
        for r in range(slot // block):
            sub = turned[r * block : (r + 1) * block]
            first_col = sub[:, 0:1].astype(jnp.int32)
            off_u = column_float - sub[:, 1:2]
            weight = jnp.exp2(off_u * off_u * scale)
            cols.append(jnp.where((lambda t: t.astype(jnp.uint32) < 8)(column - first_col), weight, 0.0).astype(BF16))
        spread = jnp.concatenate(cols)
        acc[...] += lax.dot_general(left, spread, NN, preferred_element_type=F32)
        return carry

    lax.fori_loop(0, sources, source_step, 0)
    out[...] = acc[...].astype(BF16).reshape(out.shape)


def on_device(spectra, positions, observed, cells, fractions, bucket_counts, chan_weights):
    rows = observed.shape[0]
    tiles = lax.axis_size(TILE)
    owners = lax.axis_size(VIS)
    slot = rows // 2
    width = GRID // tiles
    devices = tiles * owners
    mine = component_rows(spectra, positions)
    plane = ("vis_1", "tile_0")
    members = lax.axis_size(plane)
    own = lax.all_to_all(
        jnp.broadcast_to(mine[None], (members,) + mine.shape), plane, 0, 0, tiled=True
    ).reshape(members * mine.shape[0], 128)
    line = lax.axis_size("vis_0")
    here = [own] + [
        lax.ppermute(own, "vis_0", [(k, (k + step) % line) for k in range(line)])
        for step in range(1, line)
    ]
    there = lax.ppermute(jnp.concatenate(here), "tile_1", [(0, 1), (1, 0)])
    vmem = pl.BlockSpec(memory_space=pltpu.VMEM)
    sums = jax.ShapeDtypeStruct((rows, 128), F32)
    factors, cos_sum, sin_sum = pl.pallas_call(
        first_kernel,
        out_shape=(jax.ShapeDtypeStruct((rows, 128), BF16), sums, sums),
        in_specs=[vmem] * (line + 2),
        out_specs=(vmem,) * 3,
        name="predict_first",
        compiler_params=LIMIT,
    )(*here, cells, fractions)
    residual, packed = pl.pallas_call(
        second_kernel,
        out_shape=(
            jax.ShapeDtypeStruct(observed.shape, BF16),
            jax.ShapeDtypeStruct((tiles, 8, slot), F32),
        ),
        in_specs=[pl.BlockSpec(memory_space=pltpu.SMEM)] + [vmem] * 8,
        out_specs=(vmem, vmem),
        scratch_shapes=[pltpu.VMEM((8, rows), F32)],
        name="predict_second",
        compiler_params=LIMIT,
    )(
        bucket_counts, there, factors, cos_sum, sin_sum,
        cells, fractions, observed, chan_weights[None, :],
    )
    got = lax.all_to_all(packed, TILE, 0, 0, tiled=True)
    share = BAND // owners
    partial = pl.pallas_call(
        grid_kernel,
        out_shape=jax.ShapeDtypeStruct((owners, 2 * share, width), BF16),
        in_specs=[vmem],
        out_specs=vmem,
        scratch_shapes=[pltpu.VMEM((2 * BAND, width), F32)],
        name="gridding",
        compiler_params=LIMIT,
    )(got)
    parts = lax.all_to_all(partial, VIS, 0, 0, tiled=True)
    total = jnp.sum(parts.astype(F32), axis=0)
    return residual, total.reshape(share, 2, width)


def solution(mesh):
    torus = Mesh(mesh.devices.reshape(4, 8, 4, 2), ("vis_0", "vis_1", "tile_0", "tile_1"))
    return jax.shard_map(
        on_device,
        mesh=torus,
        in_specs=(
            P(None, VIS_TILE),
            P(None, VIS_TILE),
            P(VIS_TILE, None),
            P(None, VIS_TILE),
            P(None, VIS_TILE),
            P(VIS_TILE, None),
            P(),
        ),
        out_specs=(P(VIS_TILE, None), P(VIS, None, TILE)),
        check_vma=False,
    )
```

```python
import jax
import jax.numpy as jnp
from jax import lax
from jax.experimental import pallas as pl
from jax.experimental.pallas import tpu as pltpu
from jax.sharding import Mesh
from jax.sharding import PartitionSpec as P

GRID = 8192
BAND = 128
TAPS = 8
TILE = ("tile_0", "tile_1")
VIS = ("vis_0", "vis_1")
VIS_TILE = ("vis_0", "vis_1", "tile_0", "tile_1")
DIGIT_LANE = 64
F32 = jnp.float32
BF16 = jnp.bfloat16
NT = (((1,), (1,)), ((), ()))
NN = (((1,), (0,)), ((), ()))

COS_POLY = (1.41420408, -6.97764191, 5.71523647, -1.72834251)
SIN_POLY = (4.4428679, -7.30744333, 3.59478717, -0.78437159)
LIMIT = pltpu.CompilerParams(vmem_limit_bytes=24 * 2**20)
ROUND = 12582912.0


def three_parts(value):
    first = value.astype(BF16).astype(F32)
    rest = value - first
    second = rest.astype(BF16).astype(F32)
    return [first, second, rest - second]


def component_rows(spectra, positions):
    low = ((positions + 64) & 127) - 64
    high = (positions - low) >> 7
    digits = jnp.concatenate(
        [
            jnp.broadcast_to(d[None], (n, d.shape[0]))
            for d, n in ((high[0], 4), (low[0], 5), (high[1], 4), (low[1], 5))
        ]
    ).astype(BF16)
    rows = jnp.concatenate([spectra, digits])
    return jnp.pad(rows, ((0, 128 - rows.shape[0]), (0, 0))).T


def row_factors(cells, fractions):
    parts = []
    for axis in range(2):
        first = cells[axis : axis + 1] + 3
        low = ((first + 32) & 63) - 32
        high = first - low
        frac = three_parts(fractions[axis : axis + 1])
        parts += [low.astype(F32) * (128.0 / GRID)] + [f * (128.0 / GRID) for f in frac]
        high = ((high + GRID // 2) & (GRID - 1)) - GRID // 2
        parts += [high.astype(F32) * (1.0 / GRID), low.astype(F32) * (1.0 / GRID)]
        parts += [f * (1.0 / GRID) for f in frac]
    return parts


def monic(coefficients, s):
    lead = coefficients[-1]
    result = s + coefficients[-2] / lead
    for c in coefficients[-3::-1]:
        result = result * s + c / lead
    return result


def polynomial(coefficients, s):
    result = coefficients[-1] * s + coefficients[-2]
    for c in coefficients[-3::-1]:
        result = result * s + c
    return result


def add_products(left, comps, cos_sum, sin_sum):
    comp_block = 256
    for first in range(0, comps.shape[0], comp_block):
        piece = comps[first : first + comp_block, :]
        turns = lax.dot_general(left, piece, NT, preferred_element_type=F32)
        y = turns - ((turns + ROUND) - ROUND)
        s = y * y
        c = monic(COS_POLY, s)
        d = monic(SIN_POLY, s) * y
        cosine = (1.0 / SIN_POLY[-1] ** 2 - d * d).astype(BF16)
        sine = (c * d).astype(BF16)
        cos_sum += lax.dot_general(cosine, piece, NN, preferred_element_type=F32)
        sin_sum += lax.dot_general(sine, piece, NN, preferred_element_type=F32)
    return cos_sum, sin_sum


def first_kernel(*refs):
    pieces, (cells, fractions, factors, cos_out, sin_out) = refs[:-5], refs[-5:]
    rows = factors.shape[0]
    parts = row_factors(cells[...], fractions[...])
    lead = jnp.zeros((DIGIT_LANE, rows), F32)
    tail = jnp.zeros((128 - DIGIT_LANE - len(parts), rows), F32)
    left = jnp.concatenate([lead] + parts + [tail]).T.astype(BF16)
    factors[...] = left
    cos_sum = jnp.zeros((rows, 128), F32)
    sin_sum = jnp.zeros((rows, 128), F32)
    for comps in pieces:
        cos_sum, sin_sum = add_products(left, comps, cos_sum, sin_sum)
    cos_out[...] = cos_sum
    sin_out[...] = sin_sum


def second_kernel(
    counts, comps, factors, cos_in, sin_in, cells, fractions, observed, weights, residual, packed, fields
):
    rows = observed.shape[0]
    owners, tiles, _, slot = packed.shape
    start = []
    total = counts[0, 0] * 0
    for t in range(tiles):
        start.append(total)
        total = total + counts[0, t]

    w = weights[...]
    both = jnp.concatenate([w, w], axis=1)
    lane = lax.broadcasted_iota(jnp.int32, both.shape, 1)
    w_re = three_parts(jnp.where(lane < 64, both, 0.0))
    w_im = three_parts(jnp.where(lane < 64, 0.0, both))
    w_rows = jnp.concatenate(w_re + w_im + [jnp.zeros((2, 128), F32)]).astype(BF16)

    cos_sum, sin_sum = add_products(factors[...], comps, cos_in[...], sin_in[...])
    lanes = lax.broadcasted_iota(jnp.int32, (rows, 128), 1)
    index = lax.broadcasted_iota(jnp.int32, (rows, 128), 0)
    real = cos_sum * SIN_POLY[-1] ** 2
    imag = pltpu.roll(sin_sum, 64, 1) * (-COS_POLY[-1] * SIN_POLY[-1])
    predicted = jnp.where(lanes < 64, real, imag)
    res = jnp.where(index < total, observed[...].astype(F32) - predicted, 0.0).astype(BF16)
    residual[...] = res
    sums = lax.dot_general(w_rows, res, NT, preferred_element_type=F32)
    fields[0:1, :] = sums[0:1] + sums[1:2] + sums[2:3]
    fields[1:2, :] = sums[3:4] + sums[4:5] + sums[5:6]
    fields[2:4, :] = cells[...].astype(F32) + 0.5 * fractions[...]
    fields[4:8, :] = jnp.zeros((4, rows), F32)
    everything = fields[...]
    row_of = lax.broadcasted_iota(jnp.int32, (4, slot), 0)
    place = lax.broadcasted_iota(jnp.int32, (4, slot), 1)
    for t in range(tiles):
        moved = pltpu.roll(everything, (rows - start[t]) & (rows - 1), 1)[:4, :slot]
        moved = jnp.where((row_of >= 2) | (place < counts[0, t]), moved, 0.0)
        for owner in range(owners):
            base = float((t * owners + owner) * (GRID // (tiles * owners)))
            packed[owner, t] = moved - jnp.where(row_of == 2, base, 0.0)


def grid_kernel(got, out, acc):
    sources, _, slot = got.shape
    group = 8
    count = group * slot
    width = out.shape[2]
    scale = -0.7213475204444817
    first_line = lax.broadcasted_iota(jnp.int32, (BAND, count), 0)
    line_float = first_line.astype(F32)
    column = lax.broadcasted_iota(jnp.int32, (width, count), 0)
    column_float = column.astype(F32)
    acc[...] = jnp.zeros(acc.shape, F32)

    def step(number, carry):
        data = jnp.concatenate([got[number * group + k] for k in range(group)], axis=1)
        row_start = jnp.floor(data[3:4])
        row_centre = 3.0 - row_start + 2.0 * data[3:4]
        off = line_float - row_centre
        near = (first_line - row_start.astype(jnp.int32)).astype(jnp.uint32) < 8
        kernel = jnp.where(near, jnp.exp2(off * off * scale), 0.0)
        left = jnp.concatenate([(data[0:1] * kernel).astype(BF16), (data[1:2] * kernel).astype(BF16)])
        col_start = jnp.floor(data[2:3])
        col_centre = 3.0 - col_start + 2.0 * data[2:3]
        off_u = column_float - col_centre
        near_u = (column - col_start.astype(jnp.int32)).astype(jnp.uint32) < 8
        spread = jnp.where(near_u, jnp.exp2(off_u * off_u * scale), 0.0).astype(BF16)
        acc[...] += lax.dot_general(left, spread, NT, preferred_element_type=F32)
        return carry

    lax.fori_loop(0, sources // group, step, 0)
    upper = lax.broadcasted_iota(jnp.int32, (8, width), 0) < 4
    for g in range(BAND // 8):
        real = acc[8 * g : 8 * g + 8]
        imag = acc[BAND + 8 * g : BAND + 8 * g + 8]
        out[2 * g] = jnp.where(upper, real, pltpu.roll(imag, 4, 0)).astype(BF16)
        out[2 * g + 1] = jnp.where(upper, pltpu.roll(real, 4, 0), imag).astype(BF16)


def sum_kernel(got, out):
    blocks, sources, lines, width = got.shape
    share = lines // 2
    for b in range(blocks):
        total = jnp.sum(got[b].astype(F32), axis=0)
        for c in range(2):
            for j in range(share):
                out[j, c : c + 1, b * width : (b + 1) * width] = total[c * share + j : c * share + j + 1]


def on_device(spectra, positions, observed, cells, fractions, bucket_counts, chan_weights):
    rows = observed.shape[0]
    tiles = lax.axis_size(TILE)
    owners = lax.axis_size(VIS)
    slot = rows // 2
    width = GRID // tiles
    devices = tiles * owners
    mine = component_rows(spectra, positions)
    plane = ("vis_1", "tile_0")
    members = lax.axis_size(plane)
    own = lax.all_to_all(
        jnp.broadcast_to(mine[None], (members,) + mine.shape), plane, 0, 0, tiled=True
    ).reshape(members * mine.shape[0], 128)
    line = lax.axis_size("vis_0")
    here = [own] + [
        lax.ppermute(own, "vis_0", [(k, (k + step) % line) for k in range(line)])
        for step in range(1, line)
    ]
    there = lax.ppermute(jnp.concatenate(here), "tile_1", [(0, 1), (1, 0)])
    vmem = pl.BlockSpec(memory_space=pltpu.VMEM)
    sums = jax.ShapeDtypeStruct((rows, 128), F32)
    factors, cos_sum, sin_sum = pl.pallas_call(
        first_kernel,
        out_shape=(jax.ShapeDtypeStruct((rows, 128), BF16), sums, sums),
        in_specs=[vmem] * (line + 2),
        out_specs=(vmem,) * 3,
        name="predict_first",
        compiler_params=LIMIT,
    )(*here, cells, fractions)
    residual, packed = pl.pallas_call(
        second_kernel,
        out_shape=(
            jax.ShapeDtypeStruct(observed.shape, BF16),
            jax.ShapeDtypeStruct((line, tiles, 4, slot), F32),
        ),
        in_specs=[pl.BlockSpec(memory_space=pltpu.SMEM)] + [vmem] * 8,
        out_specs=(vmem, vmem),
        scratch_shapes=[pltpu.VMEM((8, rows), F32)],
        name="predict_second",
        compiler_params=LIMIT,
    )(
        bucket_counts, there, factors, cos_sum, sin_sum,
        cells, fractions, observed, chan_weights[None, :],
    )
    got = lax.all_to_all(
        packed.reshape(line * tiles, 4, slot), ("vis_0",) + TILE, 0, 0, tiled=True
    )
    share = BAND // owners
    block = width // line
    partial = pl.pallas_call(
        grid_kernel,
        out_shape=jax.ShapeDtypeStruct((owners, 2 * share, block), BF16),
        in_specs=[vmem],
        out_specs=vmem,
        scratch_shapes=[pltpu.VMEM((2 * BAND, block), F32)],
        name="gridding",
        compiler_params=LIMIT,
    )(got)
    parts = lax.all_to_all(partial, VIS, 0, 0, tiled=True)
    total = pl.pallas_call(
        sum_kernel,
        out_shape=jax.ShapeDtypeStruct((share, 2, width), F32),
        in_specs=[vmem],
        out_specs=vmem,
        name="add_shares",
        compiler_params=LIMIT,
    )(parts.reshape(line, owners // line, 2 * share, block))
    return residual, total


def solution(mesh):
    torus = Mesh(mesh.devices.reshape(4, 8, 4, 2), ("vis_0", "vis_1", "tile_0", "tile_1"))
    return jax.shard_map(
        on_device,
        mesh=torus,
        in_specs=(
            P(None, VIS_TILE),
            P(None, VIS_TILE),
            P(VIS_TILE, None),
            P(None, VIS_TILE),
            P(None, VIS_TILE),
            P(VIS_TILE, None),
            P(),
        ),
        out_specs=(P(VIS_TILE, None), P(VIS, None, TILE)),
        check_vma=False,
    )
```

```python
import jax
import jax.numpy as jnp
from jax import lax
from jax.experimental import pallas as pl
from jax.experimental.pallas import tpu as pltpu
from jax.sharding import Mesh
from jax.sharding import PartitionSpec as P

GRID = 8192
BAND = 128
TAPS = 8
TILE = ("tile_0", "tile_1")
VIS = ("vis_0", "vis_1")
VIS_TILE = ("vis_0", "vis_1", "tile_0", "tile_1")
DIGIT_LANE = 64
F32 = jnp.float32
BF16 = jnp.bfloat16
NT = (((1,), (1,)), ((), ()))
NN = (((1,), (0,)), ((), ()))

COS_POLY = (1.41420408, -6.97764191, 5.71523647, -1.72834251)
SIN_POLY = (4.4428679, -7.30744333, 3.59478717, -0.78437159)
LIMIT = pltpu.CompilerParams(vmem_limit_bytes=24 * 2**20)
ROUND = 12582912.0


def three_parts(value):
    first = value.astype(BF16).astype(F32)
    rest = value - first
    second = rest.astype(BF16).astype(F32)
    return [first, second, rest - second]


def component_kernel(spectra, positions, out):
    count, channels = spectra.shape
    pixels = positions[...]
    low = ((pixels + 64) & 127) - 64
    high = (pixels - low) >> 7
    digits = jnp.concatenate(
        [high[0:1]] * 4 + [low[0:1]] * 5 + [high[1:2]] * 4 + [low[1:2]] * 5 + [high[0:1] * 0] * 14
    ).astype(F32)
    blank = jnp.zeros((digits.shape[0], 128 - count), F32)
    turned = jnp.concatenate([digits, blank], axis=1).T[:count]
    rest = jnp.zeros((count, 128 - channels - turned.shape[1]), F32)
    row = jnp.concatenate([spectra[...].astype(F32), turned, rest], axis=1).astype(BF16)
    for member in range(out.shape[0]):
        out[member] = row


def row_factors(cells, fractions):
    parts = []
    for axis in range(2):
        first = cells[axis : axis + 1] + 3
        low = ((first + 32) & 63) - 32
        high = first - low
        frac = three_parts(fractions[axis : axis + 1])
        parts += [low.astype(F32) * (128.0 / GRID)] + [f * (128.0 / GRID) for f in frac]
        high = ((high + GRID // 2) & (GRID - 1)) - GRID // 2
        parts += [high.astype(F32) * (1.0 / GRID), low.astype(F32) * (1.0 / GRID)]
        parts += [f * (1.0 / GRID) for f in frac]
    return parts


def monic(coefficients, s):
    lead = coefficients[-1]
    result = s + coefficients[-2] / lead
    for c in coefficients[-3::-1]:
        result = result * s + c / lead
    return result


def polynomial(coefficients, s):
    result = coefficients[-1] * s + coefficients[-2]
    for c in coefficients[-3::-1]:
        result = result * s + c
    return result


def add_products(left, comps, cos_sum, sin_sum):
    comp_block = 256
    for first in range(0, comps.shape[0], comp_block):
        piece = comps[first : first + comp_block, :]
        turns = lax.dot_general(left, piece, NT, preferred_element_type=F32)
        y = turns - ((turns + ROUND) - ROUND)
        s = y * y
        c = monic(COS_POLY, s)
        d = monic(SIN_POLY, s) * y
        cosine = (1.0 / SIN_POLY[-1] ** 2 - d * d).astype(BF16)
        sine = (c * d).astype(BF16)
        cos_sum += lax.dot_general(cosine, piece, NN, preferred_element_type=F32)
        sin_sum += lax.dot_general(sine, piece, NN, preferred_element_type=F32)
    return cos_sum, sin_sum


def first_kernel(*refs):
    pieces, (cells, fractions, factors, cos_out, sin_out) = refs[:-5], refs[-5:]
    rows = factors.shape[0]
    parts = row_factors(cells[...], fractions[...])
    lead = jnp.zeros((DIGIT_LANE, rows), F32)
    tail = jnp.zeros((128 - DIGIT_LANE - len(parts), rows), F32)
    left = jnp.concatenate([lead] + parts + [tail]).T.astype(BF16)
    factors[...] = left
    cos_sum = jnp.zeros((rows, 128), F32)
    sin_sum = jnp.zeros((rows, 128), F32)
    for comps in pieces:
        cos_sum, sin_sum = add_products(left, comps, cos_sum, sin_sum)
    cos_out[...] = cos_sum
    sin_out[...] = sin_sum


def second_kernel(
    counts, comps, factors, cos_in, sin_in, cells, fractions, observed, weights, residual, packed, fields
):
    rows = observed.shape[0]
    owners, tiles, _, slot = packed.shape
    start = []
    total = counts[0, 0] * 0
    for t in range(tiles):
        start.append(total)
        total = total + counts[0, t]

    w = weights[...]
    both = jnp.concatenate([w, w], axis=1)
    lane = lax.broadcasted_iota(jnp.int32, both.shape, 1)
    w_re = three_parts(jnp.where(lane < 64, both, 0.0))
    w_im = three_parts(jnp.where(lane < 64, 0.0, both))
    w_rows = jnp.concatenate(w_re + w_im + [jnp.zeros((2, 128), F32)]).astype(BF16)

    cos_sum, sin_sum = add_products(factors[...], comps, cos_in[...], sin_in[...])
    lanes = lax.broadcasted_iota(jnp.int32, (rows, 128), 1)
    index = lax.broadcasted_iota(jnp.int32, (rows, 128), 0)
    real = cos_sum * SIN_POLY[-1] ** 2
    imag = pltpu.roll(sin_sum, 64, 1) * (-COS_POLY[-1] * SIN_POLY[-1])
    predicted = jnp.where(lanes < 64, real, imag)
    res = jnp.where(index < total, observed[...].astype(F32) - predicted, 0.0).astype(BF16)
    residual[...] = res
    sums = lax.dot_general(w_rows, res, NT, preferred_element_type=F32)
    fields[0:1, :] = sums[0:1] + sums[1:2] + sums[2:3]
    fields[1:2, :] = sums[3:4] + sums[4:5] + sums[5:6]
    fields[2:4, :] = cells[...].astype(F32) + 0.5 * fractions[...]
    fields[4:8, :] = jnp.zeros((4, rows), F32)
    everything = fields[...]
    row_of = lax.broadcasted_iota(jnp.int32, (4, slot), 0)
    place = lax.broadcasted_iota(jnp.int32, (4, slot), 1)
    for t in range(tiles):
        moved = pltpu.roll(everything, (rows - start[t]) & (rows - 1), 1)[:4, :slot]
        moved = jnp.where((row_of >= 2) | (place < counts[0, t]), moved, 0.0)
        for owner in range(owners):
            base = float((t * owners + owner) * (GRID // (tiles * owners)))
            packed[owner, t] = moved - jnp.where(row_of == 2, base, 0.0)


def tap_weights(position, count):
    start = jnp.floor(position)
    fraction = 2.0 * (position - start)
    first = start.astype(jnp.int32)
    lane = lax.broadcasted_iota(jnp.int32, (8, count), 0)
    tap = (lane - first) & 7
    off = (tap - 3).astype(F32) - fraction
    return jnp.exp2(off * off * -0.7213475204444817), (first + tap) >> 3


def grid_kernel(got, out, acc):
    sources, _, slot = got.shape
    group = 16
    count = group * slot
    width = out.shape[2]
    acc[...] = jnp.zeros(acc.shape, F32)
    lines = lax.broadcasted_iota(jnp.int32, (BAND // 8, 8, count), 0)
    columns = lax.broadcasted_iota(jnp.int32, (width // 8, 8, count), 0)

    def step(number, carry):
        data = jnp.concatenate([got[number * group + k] for k in range(group)], axis=1)
        weight, place = tap_weights(data[3:4], count)
        here = lines == place[None]
        left = jnp.concatenate(
            [
                jnp.where(here, (weight * data[k : k + 1])[None], 0.0).astype(BF16).reshape(BAND, count)
                for k in range(2)
            ]
        )
        weight, place = tap_weights(data[2:3], count)
        spread = jnp.where(columns == place[None], weight[None], 0.0).astype(BF16).reshape(width, count)
        acc[...] += lax.dot_general(left, spread, NT, preferred_element_type=F32)
        return carry

    lax.fori_loop(0, sources // group, step, 0)
    upper = lax.broadcasted_iota(jnp.int32, (8, width), 0) < 4
    for g in range(BAND // 8):
        real = acc[8 * g : 8 * g + 8]
        imag = acc[BAND + 8 * g : BAND + 8 * g + 8]
        out[2 * g] = jnp.where(upper, real, pltpu.roll(imag, 4, 0)).astype(BF16)
        out[2 * g + 1] = jnp.where(upper, pltpu.roll(real, 4, 0), imag).astype(BF16)


def sum_kernel(got, out):
    blocks, sources, lines, width = got.shape
    share = lines // 2
    for b in range(blocks):
        total = jnp.sum(got[b].astype(F32), axis=0)
        for c in range(2):
            for j in range(share):
                out[j, c : c + 1, b * width : (b + 1) * width] = total[c * share + j : c * share + j + 1]


def on_device(spectra, positions, observed, cells, fractions, bucket_counts, chan_weights):
    rows = observed.shape[0]
    tiles = lax.axis_size(TILE)
    owners = lax.axis_size(VIS)
    slot = rows // 2
    width = GRID // tiles
    plane = ("vis_1", "tile_0")
    members = lax.axis_size(plane)
    count = spectra.shape[1]
    vmem = pl.BlockSpec(memory_space=pltpu.VMEM)
    mine = pl.pallas_call(
        component_kernel,
        out_shape=jax.ShapeDtypeStruct((members, count, 128), BF16),
        in_specs=[vmem] * 2,
        out_specs=vmem,
        name="components",
        compiler_params=LIMIT,
    )(spectra.T, positions)
    own = lax.all_to_all(mine, plane, 0, 0, tiled=True).reshape(members * count, 128)
    line = lax.axis_size("vis_0")
    here = [own] + [
        lax.ppermute(own, "vis_0", [(k, (k + step) % line) for k in range(line)])
        for step in range(1, line)
    ]
    there = lax.ppermute(jnp.concatenate(here), "tile_1", [(0, 1), (1, 0)])
    sums = jax.ShapeDtypeStruct((rows, 128), F32)
    factors, cos_sum, sin_sum = pl.pallas_call(
        first_kernel,
        out_shape=(jax.ShapeDtypeStruct((rows, 128), BF16), sums, sums),
        in_specs=[vmem] * (line + 2),
        out_specs=(vmem,) * 3,
        name="predict_first",
        compiler_params=LIMIT,
    )(*here, cells, fractions)
    residual, packed = pl.pallas_call(
        second_kernel,
        out_shape=(
            jax.ShapeDtypeStruct(observed.shape, BF16),
            jax.ShapeDtypeStruct((line, tiles, 4, slot), F32),
        ),
        in_specs=[pl.BlockSpec(memory_space=pltpu.SMEM)] + [vmem] * 8,
        out_specs=(vmem, vmem),
        scratch_shapes=[pltpu.VMEM((8, rows), F32)],
        name="predict_second",
        compiler_params=LIMIT,
    )(
        bucket_counts, there, factors, cos_sum, sin_sum,
        cells, fractions, observed, chan_weights[None, :],
    )
    got = lax.all_to_all(
        packed.reshape(line * tiles, 4, slot), ("vis_0",) + TILE, 0, 0, tiled=True
    )
    share = BAND // owners
    block = width // line
    partial = pl.pallas_call(
        grid_kernel,
        out_shape=jax.ShapeDtypeStruct((owners, 2 * share, block), BF16),
        in_specs=[vmem],
        out_specs=vmem,
        scratch_shapes=[pltpu.VMEM((2 * BAND, block), F32)],
        name="gridding",
        compiler_params=LIMIT,
    )(got)
    parts = lax.all_to_all(partial, VIS, 0, 0, tiled=True)
    total = pl.pallas_call(
        sum_kernel,
        out_shape=jax.ShapeDtypeStruct((share, 2, width), F32),
        in_specs=[vmem],
        out_specs=vmem,
        name="add_shares",
        compiler_params=LIMIT,
    )(parts.reshape(line, owners // line, 2 * share, block))
    return residual, total


def solution(mesh):
    torus = Mesh(mesh.devices.reshape(4, 8, 4, 2), ("vis_0", "vis_1", "tile_0", "tile_1"))
    return jax.shard_map(
        on_device,
        mesh=torus,
        in_specs=(
            P(None, VIS_TILE),
            P(None, VIS_TILE),
            P(VIS_TILE, None),
            P(None, VIS_TILE),
            P(None, VIS_TILE),
            P(VIS_TILE, None),
            P(),
        ),
        out_specs=(P(VIS_TILE, None), P(VIS, None, TILE)),
        check_vma=False,
    )
```

```python
import jax
import jax.numpy as jnp
from jax import lax
from jax.experimental import pallas as pl
from jax.experimental.pallas import tpu as pltpu
from jax.sharding import Mesh
from jax.sharding import PartitionSpec as P

GRID = 8192
BAND = 128
TAPS = 8
TILE = ("tile_0", "tile_1")
VIS = ("vis_0", "vis_1")
VIS_TILE = ("vis_0", "vis_1", "tile_0", "tile_1")
DIGIT_LANE = 64
F32 = jnp.float32
BF16 = jnp.bfloat16
NT = (((1,), (1,)), ((), ()))
NN = (((1,), (0,)), ((), ()))

COS_POLY = (1.41420408, -6.97764191, 5.71523647, -1.72834251)
SIN_POLY = (4.4428679, -7.30744333, 3.59478717, -0.78437159)
LIMIT = pltpu.CompilerParams(vmem_limit_bytes=24 * 2**20)
ROUND = 12582912.0


def three_parts(value):
    first = value.astype(BF16).astype(F32)
    rest = value - first
    second = rest.astype(BF16).astype(F32)
    return [first, second, rest - second]


def component_kernel(spectra, positions, counts, out, near_counts):
    near_counts[...] = counts[...]
    count, channels = spectra.shape
    pixels = positions[...]
    low = ((pixels + 64) & 127) - 64
    high = (pixels - low) >> 7
    digits = jnp.concatenate(
        [high[0:1]] * 4 + [low[0:1]] * 5 + [high[1:2]] * 4 + [low[1:2]] * 5 + [high[0:1] * 0] * 14
    ).astype(F32)
    blank = jnp.zeros((digits.shape[0], 128 - count), F32)
    turned = jnp.concatenate([digits, blank], axis=1).T[:count]
    rest = jnp.zeros((count, 128 - channels - turned.shape[1]), F32)
    row = jnp.concatenate([spectra[...].astype(F32), turned, rest], axis=1).astype(BF16)
    for member in range(out.shape[0]):
        out[member] = row


def row_factors(cells, fractions):
    parts = []
    for axis in range(2):
        first = cells[axis : axis + 1] + 3
        low = ((first + 32) & 63) - 32
        high = first - low
        frac = three_parts(fractions[axis : axis + 1])
        parts += [low.astype(F32) * (128.0 / GRID)] + [f * (128.0 / GRID) for f in frac]
        high = ((high + GRID // 2) & (GRID - 1)) - GRID // 2
        parts += [high.astype(F32) * (1.0 / GRID), low.astype(F32) * (1.0 / GRID)]
        parts += [f * (1.0 / GRID) for f in frac]
    return parts


def monic(coefficients, s):
    lead = coefficients[-1]
    result = s + coefficients[-2] / lead
    for c in coefficients[-3::-1]:
        result = result * s + c / lead
    return result


def polynomial(coefficients, s):
    result = coefficients[-1] * s + coefficients[-2]
    for c in coefficients[-3::-1]:
        result = result * s + c
    return result


def add_products(left, comps, cos_sum, sin_sum):
    comp_block = 256
    for first in range(0, comps.shape[0], comp_block):
        piece = comps[first : first + comp_block, :]
        turns = lax.dot_general(left, piece, NT, preferred_element_type=F32)
        y = turns - ((turns + ROUND) - ROUND)
        s = y * y
        c = monic(COS_POLY, s)
        d = monic(SIN_POLY, s) * y
        cosine = (1.0 / SIN_POLY[-1] ** 2 - d * d).astype(BF16)
        sine = (c * d).astype(BF16)
        cos_sum += lax.dot_general(cosine, piece, NN, preferred_element_type=F32)
        sin_sum += lax.dot_general(sine, piece, NN, preferred_element_type=F32)
    return cos_sum, sin_sum


def first_kernel(*refs):
    pieces, rest = refs[:-7], refs[-7:]
    cells, fractions, weights, factors, cos_out, sin_out, weight_rows = rest
    w = weights[...]
    both = jnp.concatenate([w, w], axis=1)
    lane = lax.broadcasted_iota(jnp.int32, both.shape, 1)
    w_re = three_parts(jnp.where(lane < 64, both, 0.0))
    w_im = three_parts(jnp.where(lane < 64, 0.0, both))
    weight_rows[...] = jnp.concatenate(w_re + w_im + [jnp.zeros((2, 128), F32)]).astype(BF16)
    rows = factors.shape[0]
    parts = row_factors(cells[...], fractions[...])
    lead = jnp.zeros((DIGIT_LANE, rows), F32)
    tail = jnp.zeros((128 - DIGIT_LANE - len(parts), rows), F32)
    left = jnp.concatenate([lead] + parts + [tail]).T.astype(BF16)
    factors[...] = left
    cos_sum = jnp.zeros((rows, 128), F32)
    sin_sum = jnp.zeros((rows, 128), F32)
    for comps in pieces:
        cos_sum, sin_sum = add_products(left, comps, cos_sum, sin_sum)
    cos_out[...] = cos_sum
    sin_out[...] = sin_sum


def second_kernel(counts, *refs):
    pieces, rest = refs[:-10], refs[-10:]
    factors, cos_in, sin_in, cells, fractions, observed, weights, residual, packed, fields = rest
    rows = observed.shape[0]
    owners, tiles, _, slot = packed.shape
    start = []
    total = counts[0, 0] * 0
    for t in range(tiles):
        start.append(total)
        total = total + counts[0, t]

    cos_sum, sin_sum = cos_in[...], sin_in[...]
    for comps in pieces:
        cos_sum, sin_sum = add_products(factors[...], comps, cos_sum, sin_sum)
    lanes = lax.broadcasted_iota(jnp.int32, (rows, 128), 1)
    index = lax.broadcasted_iota(jnp.int32, (rows, 128), 0)
    real = cos_sum * SIN_POLY[-1] ** 2
    imag = pltpu.roll(sin_sum, 64, 1) * (-COS_POLY[-1] * SIN_POLY[-1])
    predicted = jnp.where(lanes < 64, real, imag)
    res = jnp.where(index < total, observed[...].astype(F32) - predicted, 0.0).astype(BF16)
    residual[...] = res
    sums = lax.dot_general(weights[...], res, NT, preferred_element_type=F32)
    fields[0:1, :] = sums[0:1] + sums[1:2] + sums[2:3]
    fields[1:2, :] = sums[3:4] + sums[4:5] + sums[5:6]
    fields[2:4, :] = cells[...].astype(F32) + 0.5 * fractions[...]
    fields[4:8, :] = jnp.zeros((4, rows), F32)
    everything = fields[...]
    row_of = lax.broadcasted_iota(jnp.int32, (4, slot), 0)
    place = lax.broadcasted_iota(jnp.int32, (4, slot), 1)
    for t in range(tiles):
        moved = pltpu.roll(everything, (rows - start[t]) & (rows - 1), 1)[:4, :slot]
        moved = jnp.where((row_of >= 2) | (place < counts[0, t]), moved, 0.0)
        for owner in range(owners):
            base = float((t * owners + owner) * (GRID // (tiles * owners)))
            packed[owner, t] = moved - jnp.where(row_of == 2, base, 0.0)


def tap_weights(position, count):
    start = jnp.floor(position)
    fraction = 2.0 * (position - start)
    first = start.astype(jnp.int32)
    lane = lax.broadcasted_iota(jnp.int32, (8, count), 0)
    tap = (lane - first) & 7
    off = (tap - 3).astype(F32) - fraction
    return jnp.exp2(off * off * -0.7213475204444817), (first + tap) >> 3


def grid_kernel(got, near, out, far, acc, sem):
    leave = pltpu.make_async_copy(near, far, sem)
    leave.start()
    sources, _, slot = got.shape
    group = 16
    count = group * slot
    width = out.shape[2]
    acc[...] = jnp.zeros(acc.shape, F32)
    lines = lax.broadcasted_iota(jnp.int32, (BAND // 8, 8, count), 0)
    columns = lax.broadcasted_iota(jnp.int32, (width // 8, 8, count), 0)

    def step(number, carry):
        data = jnp.concatenate([got[number * group + k] for k in range(group)], axis=1)
        weight, place = tap_weights(data[3:4], count)
        here = lines == place[None]
        left = jnp.concatenate(
            [
                jnp.where(here, (weight * data[k : k + 1])[None], 0.0).astype(BF16).reshape(BAND, count)
                for k in range(2)
            ]
        )
        weight, place = tap_weights(data[2:3], count)
        spread = jnp.where(columns == place[None], weight[None], 0.0).astype(BF16).reshape(width, count)
        acc[...] += lax.dot_general(left, spread, NT, preferred_element_type=F32)
        return carry

    lax.fori_loop(0, sources // group, step, 0)
    upper = lax.broadcasted_iota(jnp.int32, (8, width), 0) < 4
    for g in range(BAND // 8):
        real = acc[8 * g : 8 * g + 8]
        imag = acc[BAND + 8 * g : BAND + 8 * g + 8]
        out[2 * g] = jnp.where(upper, real, pltpu.roll(imag, 4, 0)).astype(BF16)
        out[2 * g + 1] = jnp.where(upper, pltpu.roll(real, 4, 0), imag).astype(BF16)
    leave.wait()


def sum_kernel(got, out):
    blocks, sources, lines, width = got.shape
    share = lines // 2
    for b in range(blocks):
        total = jnp.sum(got[b].astype(F32), axis=0)
        for c in range(2):
            for j in range(share):
                out[j, c : c + 1, b * width : (b + 1) * width] = total[c * share + j : c * share + j + 1]


def on_device(spectra, positions, observed, cells, fractions, bucket_counts, chan_weights):
    rows = observed.shape[0]
    tiles = lax.axis_size(TILE)
    owners = lax.axis_size(VIS)
    slot = rows // 2
    width = GRID // tiles
    plane = VIS + ("tile_0",)
    members = lax.axis_size(plane)
    count = spectra.shape[1]
    line = lax.axis_size("vis_0")
    vmem = pl.BlockSpec(memory_space=pltpu.VMEM)
    far = pl.BlockSpec(memory_space=pltpu.HBM)
    mine, near_counts = pl.pallas_call(
        component_kernel,
        out_shape=(
            jax.ShapeDtypeStruct((members, count, 128), BF16),
            jax.ShapeDtypeStruct(bucket_counts.shape, jnp.int32),
        ),
        in_specs=[vmem] * 3,
        out_specs=(vmem,) * 2,
        name="components",
        compiler_params=LIMIT,
    )(spectra.T, positions, bucket_counts)
    own = lax.all_to_all(mine, plane, 0, 0, tiled=True).reshape(members * count, 128)
    here = [own]
    there = [lax.ppermute(own, "tile_1", [(0, 1), (1, 0)])]
    sums = jax.ShapeDtypeStruct((rows, 128), F32)
    factors, cos_sum, sin_sum, weight_rows = pl.pallas_call(
        first_kernel,
        out_shape=(
            jax.ShapeDtypeStruct((rows, 128), BF16),
            sums,
            sums,
            jax.ShapeDtypeStruct((8, 128), BF16),
        ),
        in_specs=[vmem] * (len(here) + 3),
        out_specs=(vmem,) * 4,
        name="predict_first",
        compiler_params=LIMIT,
    )(*here, cells, fractions, chan_weights[None, :])
    near_residual, packed = pl.pallas_call(
        second_kernel,
        out_shape=(
            jax.ShapeDtypeStruct(observed.shape, BF16),
            jax.ShapeDtypeStruct((line, tiles, 4, slot), F32),
        ),
        in_specs=[pl.BlockSpec(memory_space=pltpu.SMEM)] + [vmem] * (7 + len(there)),
        out_specs=(vmem, vmem),
        scratch_shapes=[pltpu.VMEM((8, rows), F32)],
        name="predict_second",
        compiler_params=LIMIT,
    )(
        near_counts, *there, factors, cos_sum, sin_sum,
        cells, fractions, observed, weight_rows,
    )
    got = lax.all_to_all(
        packed.reshape(line * tiles, 4, slot), ("vis_0",) + TILE, 0, 0, tiled=True
    )
    share = BAND // owners
    block = width // line
    partial, residual = pl.pallas_call(
        grid_kernel,
        out_shape=(
            jax.ShapeDtypeStruct((owners, 2 * share, block), BF16),
            jax.ShapeDtypeStruct(observed.shape, BF16),
        ),
        in_specs=[vmem] * 2,
        out_specs=(vmem, far),
        scratch_shapes=[pltpu.VMEM((2 * BAND, block), F32), pltpu.SemaphoreType.DMA],
        name="gridding",
        compiler_params=LIMIT,
    )(got, near_residual)
    parts = lax.all_to_all(partial, VIS, 0, 0, tiled=True)
    total = pl.pallas_call(
        sum_kernel,
        out_shape=jax.ShapeDtypeStruct((share, 2, width), F32),
        in_specs=[vmem],
        out_specs=vmem,
        name="add_shares",
        compiler_params=LIMIT,
    )(parts.reshape(line, owners // line, 2 * share, block))
    return residual, total


def solution(mesh):
    torus = Mesh(mesh.devices.reshape(4, 8, 4, 2), ("vis_0", "vis_1", "tile_0", "tile_1"))
    return jax.shard_map(
        on_device,
        mesh=torus,
        in_specs=(
            P(None, VIS_TILE),
            P(None, VIS_TILE),
            P(VIS_TILE, None),
            P(None, VIS_TILE),
            P(None, VIS_TILE),
            P(VIS_TILE, None),
            P(),
        ),
        out_specs=(P(VIS_TILE, None), P(VIS, None, TILE)),
        check_vma=False,
    )
```

```python
import jax
import jax.numpy as jnp
from jax import lax
from jax.experimental import pallas as pl
from jax.experimental.pallas import tpu as pltpu
from jax.sharding import Mesh
from jax.sharding import PartitionSpec as P

GRID = 8192
BAND = 128
TAPS = 8
TILE = ("tile_0", "tile_1")
LINE = ("vis_a", "vis_b")
VIS = ("vis_a", "vis_b", "vis_1")
VIS_TILE = ("vis_a", "vis_b", "vis_1", "tile_0", "tile_1")
DIGIT_LANE = 64
F32 = jnp.float32
BF16 = jnp.bfloat16
NT = (((1,), (1,)), ((), ()))
NN = (((1,), (0,)), ((), ()))

COS_POLY = (1.41420408, -6.97764191, 5.71523647, -1.72834251)
SIN_POLY = (4.4428679, -7.30744333, 3.59478717, -0.78437159)
LIMIT = pltpu.CompilerParams(vmem_limit_bytes=24 * 2**20)
ROUND = 12582912.0


def three_parts(value):
    first = value.astype(BF16).astype(F32)
    rest = value - first
    second = rest.astype(BF16).astype(F32)
    return [first, second, rest - second]


def component_kernel(spectra, positions, counts, out, near_counts):
    near_counts[...] = counts[...]
    count, channels = spectra.shape
    pixels = positions[...]
    low = ((pixels + 64) & 127) - 64
    high = (pixels - low) >> 7
    digits = jnp.concatenate(
        [high[0:1]] * 4 + [low[0:1]] * 5 + [high[1:2]] * 4 + [low[1:2]] * 5 + [high[0:1] * 0] * 14
    ).astype(F32)
    blank = jnp.zeros((digits.shape[0], 128 - count), F32)
    turned = jnp.concatenate([digits, blank], axis=1).T[:count]
    rest = jnp.zeros((count, 128 - channels - turned.shape[1]), F32)
    row = jnp.concatenate([spectra[...].astype(F32), turned, rest], axis=1).astype(BF16)
    for member in range(out.shape[0]):
        out[member] = row


def row_factors(cells, fractions):
    parts = []
    for axis in range(2):
        first = cells[axis : axis + 1] + 3
        low = ((first + 32) & 63) - 32
        high = first - low
        frac = three_parts(fractions[axis : axis + 1])
        parts += [low.astype(F32) * (128.0 / GRID)] + [f * (128.0 / GRID) for f in frac]
        high = ((high + GRID // 2) & (GRID - 1)) - GRID // 2
        parts += [high.astype(F32) * (1.0 / GRID), low.astype(F32) * (1.0 / GRID)]
        parts += [f * (1.0 / GRID) for f in frac]
    return parts


def monic(coefficients, s):
    lead = coefficients[-1]
    result = s + coefficients[-2] / lead
    for c in coefficients[-3::-1]:
        result = result * s + c / lead
    return result


def polynomial(coefficients, s):
    result = coefficients[-1] * s + coefficients[-2]
    for c in coefficients[-3::-1]:
        result = result * s + c
    return result


def add_products(left, comps, cos_sum, sin_sum):
    comp_block = 512
    for first in range(0, comps.shape[0], comp_block):
        piece = comps[first : first + comp_block, :]
        turns = lax.dot_general(left, piece, NT, preferred_element_type=F32)
        y = turns - ((turns + ROUND) - ROUND)
        s = y * y
        c = monic(COS_POLY, s)
        d = monic(SIN_POLY, s) * y
        cosine = (1.0 / SIN_POLY[-1] ** 2 - d * d).astype(BF16)
        sine = (c * d).astype(BF16)
        cos_sum += lax.dot_general(cosine, piece, NN, preferred_element_type=F32)
        sin_sum += lax.dot_general(sine, piece, NN, preferred_element_type=F32)
    return cos_sum, sin_sum


def first_kernel(*refs):
    pieces, rest = refs[:-7], refs[-7:]
    cells, fractions, weights, factors, cos_out, sin_out, weight_rows = rest
    w = weights[...]
    both = jnp.concatenate([w, w], axis=1)
    lane = lax.broadcasted_iota(jnp.int32, both.shape, 1)
    w_re = three_parts(jnp.where(lane < 64, both, 0.0))
    w_im = three_parts(jnp.where(lane < 64, 0.0, both))
    weight_rows[...] = jnp.concatenate(w_re + w_im + [jnp.zeros((2, 128), F32)]).astype(BF16)
    rows = factors.shape[0]
    parts = row_factors(cells[...], fractions[...])
    lead = jnp.zeros((DIGIT_LANE, rows), F32)
    tail = jnp.zeros((128 - DIGIT_LANE - len(parts), rows), F32)
    left = jnp.concatenate([lead] + parts + [tail]).T.astype(BF16)
    factors[...] = left
    cos_sum = jnp.zeros((rows, 128), F32)
    sin_sum = jnp.zeros((rows, 128), F32)
    for comps in pieces:
        cos_sum, sin_sum = add_products(left, comps, cos_sum, sin_sum)
    cos_out[...] = cos_sum
    sin_out[...] = sin_sum


def middle_kernel(*refs):
    pieces, (factors, cos_in, sin_in, cos_out, sin_out) = refs[:-5], refs[-5:]
    cos_sum, sin_sum = cos_in[...], sin_in[...]
    for comps in pieces:
        cos_sum, sin_sum = add_products(factors[...], comps, cos_sum, sin_sum)
    cos_out[...] = cos_sum
    sin_out[...] = sin_sum


def second_kernel(counts, *refs):
    pieces, rest = refs[:-10], refs[-10:]
    factors, cos_in, sin_in, cells, fractions, observed, weights, residual, packed, fields = rest
    rows = observed.shape[0]
    owners, tiles, _, slot = packed.shape
    start = []
    total = counts[0, 0] * 0
    for t in range(tiles):
        start.append(total)
        total = total + counts[0, t]

    cos_sum, sin_sum = cos_in[...], sin_in[...]
    for comps in pieces:
        cos_sum, sin_sum = add_products(factors[...], comps, cos_sum, sin_sum)
    lanes = lax.broadcasted_iota(jnp.int32, (rows, 128), 1)
    index = lax.broadcasted_iota(jnp.int32, (rows, 128), 0)
    real = cos_sum * SIN_POLY[-1] ** 2
    imag = pltpu.roll(sin_sum, 64, 1) * (-COS_POLY[-1] * SIN_POLY[-1])
    predicted = jnp.where(lanes < 64, real, imag)
    res = jnp.where(index < total, observed[...].astype(F32) - predicted, 0.0).astype(BF16)
    residual[...] = res
    sums = lax.dot_general(weights[...], res, NT, preferred_element_type=F32)
    fields[0:1, :] = sums[0:1] + sums[1:2] + sums[2:3]
    fields[1:2, :] = sums[3:4] + sums[4:5] + sums[5:6]
    fields[2:4, :] = cells[...].astype(F32) + 0.5 * fractions[...]
    fields[4:8, :] = jnp.zeros((4, rows), F32)
    everything = fields[...]
    row_of = lax.broadcasted_iota(jnp.int32, (4, slot), 0)
    place = lax.broadcasted_iota(jnp.int32, (4, slot), 1)
    for t in range(tiles):
        moved = pltpu.roll(everything, (rows - start[t]) & (rows - 1), 1)[:4, :slot]
        moved = jnp.where((row_of >= 2) | (place < counts[0, t]), moved, 0.0)
        for owner in range(owners):
            base = float((t * owners + owner) * (GRID // (tiles * owners)))
            packed[owner, t] = moved - jnp.where(row_of == 2, base, 0.0)


def tap_weights(position, count):
    start = jnp.floor(position)
    fraction = 2.0 * (position - start)
    first = start.astype(jnp.int32)
    lane = lax.broadcasted_iota(jnp.int32, (8, count), 0)
    tap = (lane - first) & 7
    off = (tap - 3).astype(F32) - fraction
    return jnp.exp2(off * off * -0.7213475204444817), (first + tap) >> 3


def grid_kernel(got, near, out, far, acc, sem):
    leave = pltpu.make_async_copy(near, far, sem)
    leave.start()
    sources, _, slot = got.shape
    group = 16
    count = group * slot
    width = out.shape[2]
    acc[...] = jnp.zeros(acc.shape, F32)
    lines = lax.broadcasted_iota(jnp.int32, (BAND // 8, 8, count), 0)
    columns = lax.broadcasted_iota(jnp.int32, (width // 8, 8, count), 0)

    def step(number, carry):
        data = jnp.concatenate([got[number * group + k] for k in range(group)], axis=1)
        weight, place = tap_weights(data[3:4], count)
        here = lines == place[None]
        left = jnp.concatenate(
            [
                jnp.where(here, (weight * data[k : k + 1])[None], 0.0).astype(BF16).reshape(BAND, count)
                for k in range(2)
            ]
        )
        weight, place = tap_weights(data[2:3], count)
        spread = jnp.where(columns == place[None], weight[None], 0.0).astype(BF16).reshape(width, count)
        acc[...] += lax.dot_general(left, spread, NT, preferred_element_type=F32)
        return carry

    lax.fori_loop(0, sources // group, step, 0)
    upper = lax.broadcasted_iota(jnp.int32, (8, width), 0) < 4
    for g in range(BAND // 8):
        real = acc[8 * g : 8 * g + 8]
        imag = acc[BAND + 8 * g : BAND + 8 * g + 8]
        out[2 * g] = jnp.where(upper, real, pltpu.roll(imag, 4, 0)).astype(BF16)
        out[2 * g + 1] = jnp.where(upper, pltpu.roll(real, 4, 0), imag).astype(BF16)
    leave.wait()


def sum_kernel(got, out):
    blocks, sources, lines, width = got.shape
    share = lines // 2
    for b in range(blocks):
        total = jnp.sum(got[b].astype(F32), axis=0)
        for c in range(2):
            for j in range(share):
                out[j, c : c + 1, b * width : (b + 1) * width] = total[c * share + j : c * share + j + 1]


def on_device(spectra, positions, observed, cells, fractions, bucket_counts, chan_weights):
    rows = observed.shape[0]
    tiles = lax.axis_size(TILE)
    owners = lax.axis_size(VIS)
    slot = rows // 2
    width = GRID // tiles
    plane = ("vis_a", "vis_1", "tile_0")
    members = lax.axis_size(plane)
    count = spectra.shape[1]
    line = lax.axis_size(LINE)
    vmem = pl.BlockSpec(memory_space=pltpu.VMEM)
    far = pl.BlockSpec(memory_space=pltpu.HBM)
    mine, near_counts = pl.pallas_call(
        component_kernel,
        out_shape=(
            jax.ShapeDtypeStruct((members, count, 128), BF16),
            jax.ShapeDtypeStruct(bucket_counts.shape, jnp.int32),
        ),
        in_specs=[vmem] * 3,
        out_specs=(vmem,) * 2,
        name="components",
        compiler_params=LIMIT,
    )(spectra.T, positions, bucket_counts)
    own = lax.all_to_all(mine, plane, 0, 0, tiled=True).reshape(members * count, 128)
    swap = [(0, 1), (1, 0)]
    here = [own]
    next_to = lax.ppermute(own, "vis_b", swap)
    other = lax.ppermute(own, "tile_1", swap)
    sums = jax.ShapeDtypeStruct((rows, 128), F32)
    factors, cos_sum, sin_sum, weight_rows = pl.pallas_call(
        first_kernel,
        out_shape=(
            jax.ShapeDtypeStruct((rows, 128), BF16),
            sums,
            sums,
            jax.ShapeDtypeStruct((8, 128), BF16),
        ),
        in_specs=[vmem] * (len(here) + 3),
        out_specs=(vmem,) * 4,
        name="predict_first",
        compiler_params=LIMIT,
    )(*here, cells, fractions, chan_weights[None, :])
    middle = pl.pallas_call(
        middle_kernel,
        out_shape=(sums, sums),
        in_specs=[vmem] * 4,
        out_specs=(vmem, vmem),
        name="predict_middle",
        compiler_params=LIMIT,
    )
    cos_sum, sin_sum = middle(other, factors, cos_sum, sin_sum)
    next_to, cos_sum, sin_sum = lax.optimization_barrier((next_to, cos_sum, sin_sum))
    there = [lax.ppermute(next_to, "tile_1", swap)]
    cos_sum, sin_sum = middle(next_to, factors, cos_sum, sin_sum)
    near_residual, packed = pl.pallas_call(
        second_kernel,
        out_shape=(
            jax.ShapeDtypeStruct(observed.shape, BF16),
            jax.ShapeDtypeStruct((line, tiles, 4, slot), F32),
        ),
        in_specs=[pl.BlockSpec(memory_space=pltpu.SMEM)] + [vmem] * 8,
        out_specs=(vmem, vmem),
        scratch_shapes=[pltpu.VMEM((8, rows), F32)],
        name="predict_second",
        compiler_params=LIMIT,
    )(
        near_counts, *there, factors, cos_sum, sin_sum,
        cells, fractions, observed, weight_rows,
    )
    got = lax.all_to_all(
        packed.reshape(line * tiles, 4, slot), LINE + TILE, 0, 0, tiled=True
    )
    share = BAND // owners
    block = width // line
    partial, residual = pl.pallas_call(
        grid_kernel,
        out_shape=(
            jax.ShapeDtypeStruct((owners, 2 * share, block), BF16),
            jax.ShapeDtypeStruct(observed.shape, BF16),
        ),
        in_specs=[vmem] * 2,
        out_specs=(vmem, far),
        scratch_shapes=[pltpu.VMEM((2 * BAND, block), F32), pltpu.SemaphoreType.DMA],
        name="gridding",
        compiler_params=LIMIT,
    )(got, near_residual)
    parts = lax.all_to_all(partial, VIS, 0, 0, tiled=True)
    total = pl.pallas_call(
        sum_kernel,
        out_shape=jax.ShapeDtypeStruct((share, 2, width), F32),
        in_specs=[vmem],
        out_specs=vmem,
        name="add_shares",
        compiler_params=LIMIT,
    )(parts.reshape(line, owners // line, 2 * share, block))
    return residual, total


def solution(mesh):
    torus = Mesh(mesh.devices.reshape(2, 2, 8, 4, 2), VIS_TILE)
    return jax.shard_map(
        on_device,
        mesh=torus,
        in_specs=(
            P(None, VIS_TILE),
            P(None, VIS_TILE),
            P(VIS_TILE, None),
            P(None, VIS_TILE),
            P(None, VIS_TILE),
            P(VIS_TILE, None),
            P(),
        ),
        out_specs=(P(VIS_TILE, None), P(VIS, None, TILE)),
        check_vma=False,
    )
```

```python
import jax
import jax.numpy as jnp
from jax import lax
from jax.experimental import pallas as pl
from jax.experimental.pallas import tpu as pltpu
from jax.sharding import Mesh
from jax.sharding import PartitionSpec as P

GRID = 8192
BAND = 128
TILE = ("tile_0", "tile_1")
LINE = ("vis_a", "vis_b")
VIS = ("vis_a", "vis_b", "vis_1")
VIS_TILE = ("vis_a", "vis_b", "vis_1", "tile_0", "tile_1")
DIGIT_LANE = 64
F32 = jnp.float32
BF16 = jnp.bfloat16
NT = (((1,), (1,)), ((), ()))
NN = (((1,), (0,)), ((), ()))

COS_POLY = (1.41420408, -6.97764191, 5.71523647, -1.72834251)
SIN_POLY = (4.4428679, -7.30744333, 3.59478717, -0.78437159)
LIMIT = pltpu.CompilerParams(vmem_limit_bytes=24 * 2**20)


def three_parts(value):
    first = value.astype(BF16).astype(F32)
    rest = value - first
    second = rest.astype(BF16).astype(F32)
    return [first, second, rest - second]


def component_kernel(spectra, positions, counts, out, near_counts):
    near_counts[...] = counts[...]
    count, channels = spectra.shape
    pixels = positions[...]
    low = ((pixels + 64) & 127) - 64
    high = (pixels - low) >> 7
    digits = jnp.concatenate(
        [high[0:1]] * 4 + [low[0:1]] * 5 + [high[1:2]] * 4 + [low[1:2]] * 5 + [high[0:1] * 0] * 14
    ).astype(F32)
    blank = jnp.zeros((digits.shape[0], 128 - count), F32)
    turned = jnp.concatenate([digits, blank], axis=1).T[:count]
    rest = jnp.zeros((count, 128 - channels - turned.shape[1]), F32)
    row = jnp.concatenate([spectra[...].astype(F32), turned, rest], axis=1).astype(BF16)
    for member in range(out.shape[0]):
        out[member] = row


def row_factors(cells, fractions):
    parts = []
    for axis in range(2):
        first = cells[axis : axis + 1] + 3
        low = ((first + 32) & 63) - 32
        high = first - low
        frac = three_parts(fractions[axis : axis + 1])
        parts += [low.astype(F32) * (128.0 / GRID)] + [f * (128.0 / GRID) for f in frac]
        high = ((high + GRID // 2) & (GRID - 1)) - GRID // 2
        parts += [high.astype(F32) * (1.0 / GRID), low.astype(F32) * (1.0 / GRID)]
        parts += [f * (1.0 / GRID) for f in frac]
    return parts


def monic(coefficients, s):
    lead = coefficients[-1]
    result = s + coefficients[-2] / lead
    for c in coefficients[-3::-1]:
        result = result * s + c / lead
    return result


def add_products(left, comps, cos_sum, sin_sum):
    comp_block = 512
    for first in range(0, comps.shape[0], comp_block):
        piece = comps[first : first + comp_block, :]
        turns = lax.dot_general(left, piece, NT, preferred_element_type=F32)
        y = turns - jnp.round(turns)
        s = y * y
        c = monic(COS_POLY, s)
        d = monic(SIN_POLY, s) * y
        cosine = (1.0 / SIN_POLY[-1] ** 2 - d * d).astype(BF16)
        sine = (c * d).astype(BF16)
        cos_sum += lax.dot_general(cosine, piece, NN, preferred_element_type=F32)
        sin_sum += lax.dot_general(sine, piece, NN, preferred_element_type=F32)
    return cos_sum, sin_sum


def first_kernel(*refs):
    pieces, rest = refs[:-7], refs[-7:]
    cells, fractions, weights, factors, cos_out, sin_out, weight_rows = rest
    w = weights[...]
    both = jnp.concatenate([w, w], axis=1)
    lane = lax.broadcasted_iota(jnp.int32, both.shape, 1)
    w_re = three_parts(jnp.where(lane < 64, both, 0.0))
    w_im = three_parts(jnp.where(lane < 64, 0.0, both))
    weight_rows[...] = jnp.concatenate(w_re + w_im + [jnp.zeros((2, 128), F32)]).astype(BF16)
    rows = factors.shape[0]
    parts = row_factors(cells[...], fractions[...])
    lead = jnp.zeros((DIGIT_LANE, rows), F32)
    tail = jnp.zeros((128 - DIGIT_LANE - len(parts), rows), F32)
    left = jnp.concatenate([lead] + parts + [tail]).T.astype(BF16)
    factors[...] = left
    cos_sum = jnp.zeros((rows, 128), F32)
    sin_sum = jnp.zeros((rows, 128), F32)
    for comps in pieces:
        cos_sum, sin_sum = add_products(left, comps, cos_sum, sin_sum)
    cos_out[...] = cos_sum
    sin_out[...] = sin_sum


def middle_kernel(*refs):
    pieces, (factors, cos_in, sin_in, cos_out, sin_out) = refs[:-5], refs[-5:]
    cos_sum, sin_sum = cos_in[...], sin_in[...]
    for comps in pieces:
        cos_sum, sin_sum = add_products(factors[...], comps, cos_sum, sin_sum)
    cos_out[...] = cos_sum
    sin_out[...] = sin_sum


def second_kernel(counts, *refs):
    pieces, rest = refs[:-10], refs[-10:]
    factors, cos_in, sin_in, cells, fractions, observed, weights, residual, packed, fields = rest
    rows = observed.shape[0]
    owners, tiles, _, slot = packed.shape
    start = []
    total = counts[0, 0] * 0
    for t in range(tiles):
        start.append(total)
        total = total + counts[0, t]

    cos_sum, sin_sum = cos_in[...], sin_in[...]
    for comps in pieces:
        cos_sum, sin_sum = add_products(factors[...], comps, cos_sum, sin_sum)
    lanes = lax.broadcasted_iota(jnp.int32, (rows, 128), 1)
    index = lax.broadcasted_iota(jnp.int32, (rows, 128), 0)
    real = cos_sum * SIN_POLY[-1] ** 2
    imag = pltpu.roll(sin_sum, 64, 1) * (-COS_POLY[-1] * SIN_POLY[-1])
    predicted = jnp.where(lanes < 64, real, imag)
    res = jnp.where(index < total, observed[...].astype(F32) - predicted, 0.0).astype(BF16)
    residual[...] = res
    sums = lax.dot_general(weights[...], res, NT, preferred_element_type=F32)
    fields[0:1, :] = sums[0:1] + sums[1:2] + sums[2:3]
    fields[1:2, :] = sums[3:4] + sums[4:5] + sums[5:6]
    fields[2:4, :] = cells[...].astype(F32) + 0.5 * fractions[...]
    fields[4:8, :] = jnp.zeros((4, rows), F32)
    everything = fields[...]
    row_of = lax.broadcasted_iota(jnp.int32, (4, slot), 0)
    place = lax.broadcasted_iota(jnp.int32, (4, slot), 1)
    for t in range(tiles):
        moved = pltpu.roll(everything, (rows - start[t]) & (rows - 1), 1)[:4, :slot]
        moved = jnp.where((row_of >= 2) | (place < counts[0, t]), moved, 0.0)
        for owner in range(owners):
            base = float((t * owners + owner) * (GRID // (tiles * owners)))
            packed[owner, t] = moved - jnp.where(row_of == 2, base, 0.0)


def tap_weights(position, count):
    start = jnp.floor(position)
    fraction = 2.0 * (position - start)
    first = start.astype(jnp.int32)
    lane = lax.broadcasted_iota(jnp.int32, (8, count), 0)
    tap = (lane - first) & 7
    off = (tap - 3).astype(F32) - fraction
    return jnp.exp2(off * off * -0.7213475204444817), (first + tap) >> 3


def grid_kernel(got, near, out, far, acc, sem):
    leave = pltpu.make_async_copy(near, far, sem)
    leave.start()
    sources, _, slot = got.shape
    group = 32
    count = group * slot
    width = out.shape[2]
    acc[...] = jnp.zeros(acc.shape, F32)
    lines = lax.broadcasted_iota(jnp.int32, (BAND // 8, 8, count), 0)
    columns = lax.broadcasted_iota(jnp.int32, (width // 8, 8, count), 0)

    def step(number, carry):
        data = jnp.concatenate([got[number * group + k] for k in range(group)], axis=1)
        weight, place = tap_weights(data[3:4], count)
        here = lines == place[None]
        left = jnp.concatenate(
            [
                jnp.where(here, (weight * data[k : k + 1])[None], 0.0).astype(BF16).reshape(BAND, count)
                for k in range(2)
            ]
        )
        weight, place = tap_weights(data[2:3], count)
        spread = jnp.where(columns == place[None], weight[None], 0.0).astype(BF16).reshape(width, count)
        acc[...] += lax.dot_general(left, spread, NT, preferred_element_type=F32)
        return carry

    lax.fori_loop(0, sources // group, step, 0)
    upper = lax.broadcasted_iota(jnp.int32, (8, width), 0) < 4
    for g in range(BAND // 8):
        real = acc[8 * g : 8 * g + 8]
        imag = acc[BAND + 8 * g : BAND + 8 * g + 8]
        out[2 * g] = jnp.where(upper, real, pltpu.roll(imag, 4, 0)).astype(BF16)
        out[2 * g + 1] = jnp.where(upper, pltpu.roll(real, 4, 0), imag).astype(BF16)
    leave.wait()


def sum_kernel(got, out):
    blocks, _, lines, width = got.shape
    share = lines // 2
    for b in range(blocks):
        total = jnp.sum(got[b].astype(F32), axis=0)
        for c in range(2):
            for j in range(share):
                out[j, c : c + 1, b * width : (b + 1) * width] = total[c * share + j : c * share + j + 1]


def on_device(spectra, positions, observed, cells, fractions, bucket_counts, chan_weights):
    rows = observed.shape[0]
    tiles = lax.axis_size(TILE)
    owners = lax.axis_size(VIS)
    slot = rows // 2
    width = GRID // tiles
    plane = ("vis_a", "vis_1", "tile_0")
    members = lax.axis_size(plane)
    count = spectra.shape[1]
    line = lax.axis_size(LINE)
    vmem = pl.BlockSpec(memory_space=pltpu.VMEM)
    far = pl.BlockSpec(memory_space=pltpu.HBM)
    mine, near_counts = pl.pallas_call(
        component_kernel,
        out_shape=(
            jax.ShapeDtypeStruct((members, count, 128), BF16),
            jax.ShapeDtypeStruct(bucket_counts.shape, jnp.int32),
        ),
        in_specs=[vmem] * 3,
        out_specs=(vmem,) * 2,
        name="components",
        compiler_params=LIMIT,
    )(spectra.T, positions, bucket_counts)
    own = lax.all_to_all(mine, plane, 0, 0, tiled=True).reshape(members * count, 128)
    swap = [(0, 1), (1, 0)]
    here = [own]
    next_to = lax.ppermute(own, "vis_b", swap)
    other = lax.ppermute(own, "tile_1", swap)
    sums = jax.ShapeDtypeStruct((rows, 128), F32)
    factors, cos_sum, sin_sum, weight_rows = pl.pallas_call(
        first_kernel,
        out_shape=(
            jax.ShapeDtypeStruct((rows, 128), BF16),
            sums,
            sums,
            jax.ShapeDtypeStruct((8, 128), BF16),
        ),
        in_specs=[vmem] * (len(here) + 3),
        out_specs=(vmem,) * 4,
        name="predict_first",
        compiler_params=LIMIT,
    )(*here, cells, fractions, chan_weights[None, :])
    middle = pl.pallas_call(
        middle_kernel,
        out_shape=(sums, sums),
        in_specs=[vmem] * 4,
        out_specs=(vmem, vmem),
        name="predict_middle",
        compiler_params=LIMIT,
    )
    cos_sum, sin_sum = middle(other, factors, cos_sum, sin_sum)
    next_to, cos_sum, sin_sum = lax.optimization_barrier((next_to, cos_sum, sin_sum))
    there = [lax.ppermute(next_to, "tile_1", swap)]
    cos_sum, sin_sum = middle(next_to, factors, cos_sum, sin_sum)
    near_residual, packed = pl.pallas_call(
        second_kernel,
        out_shape=(
            jax.ShapeDtypeStruct(observed.shape, BF16),
            jax.ShapeDtypeStruct((line, tiles, 4, slot), F32),
        ),
        in_specs=[pl.BlockSpec(memory_space=pltpu.SMEM)] + [vmem] * 8,
        out_specs=(vmem, vmem),
        scratch_shapes=[pltpu.VMEM((8, rows), F32)],
        name="predict_second",
        compiler_params=LIMIT,
    )(
        near_counts, *there, factors, cos_sum, sin_sum,
        cells, fractions, observed, weight_rows,
    )
    got = lax.all_to_all(
        packed.reshape(line * tiles, 4, slot), LINE + TILE, 0, 0, tiled=True
    )
    share = BAND // owners
    block = width // line
    partial, residual = pl.pallas_call(
        grid_kernel,
        out_shape=(
            jax.ShapeDtypeStruct((owners, 2 * share, block), BF16),
            jax.ShapeDtypeStruct(observed.shape, BF16),
        ),
        in_specs=[vmem] * 2,
        out_specs=(vmem, far),
        scratch_shapes=[pltpu.VMEM((2 * BAND, block), F32), pltpu.SemaphoreType.DMA],
        name="gridding",
        compiler_params=LIMIT,
    )(got, near_residual)
    parts = lax.all_to_all(partial, VIS, 0, 0, tiled=True)
    total = pl.pallas_call(
        sum_kernel,
        out_shape=jax.ShapeDtypeStruct((share, 2, width), F32),
        in_specs=[vmem],
        out_specs=vmem,
        name="add_shares",
        compiler_params=LIMIT,
    )(parts.reshape(line, owners // line, 2 * share, block))
    return residual, total


def solution(mesh):
    torus = Mesh(mesh.devices.reshape(2, 2, 8, 4, 2), VIS_TILE)
    return jax.shard_map(
        on_device,
        mesh=torus,
        in_specs=(
            P(None, VIS_TILE),
            P(None, VIS_TILE),
            P(VIS_TILE, None),
            P(None, VIS_TILE),
            P(None, VIS_TILE),
            P(VIS_TILE, None),
            P(),
        ),
        out_specs=(P(VIS_TILE, None), P(VIS, None, TILE)),
        check_vma=False,
    )
```

```python
import jax
import jax.numpy as jnp
from jax import lax
from jax.experimental import pallas as pl
from jax.experimental.pallas import tpu as pltpu
from jax.sharding import Mesh
from jax.sharding import PartitionSpec as P

GRID = 8192
BAND = 128
TILE = ("tile_0", "tile_1")
LINE = ("vis_a", "vis_b")
VIS = ("vis_a", "vis_b", "vis_1")
VIS_TILE = ("vis_a", "vis_b", "vis_1", "tile_0", "tile_1")
DIGIT_LANE = 64
F32 = jnp.float32
BF16 = jnp.bfloat16
NT = (((1,), (1,)), ((), ()))
NN = (((1,), (0,)), ((), ()))

COS_POLY = (1.41420408, -6.97764191, 5.71523647, -1.72834251)
SIN_POLY = (4.4428679, -7.30744333, 3.59478717, -0.78437159)
LIMIT = pltpu.CompilerParams(vmem_limit_bytes=24 * 2**20)


def three_parts(value):
    first = value.astype(BF16).astype(F32)
    rest = value - first
    second = rest.astype(BF16).astype(F32)
    return [first, second, rest - second]


def component_kernel(spectra, positions, counts, out, near_counts):
    near_counts[...] = counts[...]
    count, channels = spectra.shape
    pixels = positions[...]
    low = ((pixels + 64) & 127) - 64
    high = (pixels - low) >> 7
    digits = jnp.concatenate(
        [high[0:1]] * 4 + [low[0:1]] * 5 + [high[1:2]] * 4 + [low[1:2]] * 5 + [high[0:1] * 0] * 14
    ).astype(F32)
    blank = jnp.zeros((digits.shape[0], 128 - count), F32)
    turned = jnp.concatenate([digits, blank], axis=1).T[:count]
    rest = jnp.zeros((count, 128 - channels - turned.shape[1]), F32)
    row = jnp.concatenate([spectra[...].astype(F32), turned, rest], axis=1).astype(BF16)
    for member in range(out.shape[0]):
        out[member] = row


def row_factors(cells, fractions):
    parts = []
    for axis in range(2):
        first = cells[axis : axis + 1] + 3
        low = ((first + 32) & 63) - 32
        high = first - low
        frac = three_parts(fractions[axis : axis + 1])
        parts += [low.astype(F32) * (128.0 / GRID)] + [f * (128.0 / GRID) for f in frac]
        high = ((high + GRID // 2) & (GRID - 1)) - GRID // 2
        parts += [high.astype(F32) * (1.0 / GRID), low.astype(F32) * (1.0 / GRID)]
        parts += [f * (1.0 / GRID) for f in frac]
    return parts


def monic(coefficients, s):
    lead = coefficients[-1]
    result = s + coefficients[-2] / lead
    for c in coefficients[-3::-1]:
        result = result * s + c / lead
    return result


def add_products(left, comps, cos_sum, sin_sum):
    comp_block = 512
    for first in range(0, comps.shape[0], comp_block):
        piece = comps[first : first + comp_block, :]
        turns = lax.dot_general(left, piece, NT, preferred_element_type=F32)
        y = turns - jnp.round(turns)
        s = y * y
        c = monic(COS_POLY, s)
        d = monic(SIN_POLY, s) * y
        cosine = (1.0 / SIN_POLY[-1] ** 2 - d * d).astype(BF16)
        sine = (c * d).astype(BF16)
        cos_sum += lax.dot_general(cosine, piece, NN, preferred_element_type=F32)
        sin_sum += lax.dot_general(sine, piece, NN, preferred_element_type=F32)
    return cos_sum, sin_sum


def first_kernel(*refs):
    pieces, rest = refs[:-7], refs[-7:]
    cells, fractions, weights, factors, cos_out, sin_out, weight_rows = rest
    w = weights[...]
    both = jnp.concatenate([w, w], axis=1)
    lane = lax.broadcasted_iota(jnp.int32, both.shape, 1)
    w_re = three_parts(jnp.where(lane < 64, both, 0.0))
    w_im = three_parts(jnp.where(lane < 64, 0.0, both))
    weight_rows[...] = jnp.concatenate(w_re + w_im + [jnp.zeros((2, 128), F32)]).astype(BF16)
    rows = factors.shape[0]
    parts = row_factors(cells[...], fractions[...])
    lead = jnp.zeros((DIGIT_LANE, rows), F32)
    tail = jnp.zeros((128 - DIGIT_LANE - len(parts), rows), F32)
    left = jnp.concatenate([lead] + parts + [tail]).T.astype(BF16)
    factors[...] = left
    cos_sum = jnp.zeros((rows, 128), F32)
    sin_sum = jnp.zeros((rows, 128), F32)
    for comps in pieces:
        cos_sum, sin_sum = add_products(left, comps, cos_sum, sin_sum)
    cos_out[...] = cos_sum
    sin_out[...] = sin_sum


def middle_kernel(*refs):
    pieces, (factors, cos_in, sin_in, cos_out, sin_out) = refs[:-5], refs[-5:]
    cos_sum, sin_sum = cos_in[...], sin_in[...]
    for comps in pieces:
        cos_sum, sin_sum = add_products(factors[...], comps, cos_sum, sin_sum)
    cos_out[...] = cos_sum
    sin_out[...] = sin_sum


def second_kernel(counts, *refs):
    pieces, rest = refs[:-10], refs[-10:]
    factors, cos_in, sin_in, cells, fractions, observed, weights, residual, packed, fields = rest
    rows = observed.shape[0]
    owners, tiles, _, slot = packed.shape
    start = []
    total = counts[0, 0] * 0
    for t in range(tiles):
        start.append(total)
        total = total + counts[0, t]

    cos_sum, sin_sum = cos_in[...], sin_in[...]
    for comps in pieces:
        cos_sum, sin_sum = add_products(factors[...], comps, cos_sum, sin_sum)
    lanes = lax.broadcasted_iota(jnp.int32, (rows, 128), 1)
    index = lax.broadcasted_iota(jnp.int32, (rows, 128), 0)
    real = cos_sum * SIN_POLY[-1] ** 2
    imag = pltpu.roll(sin_sum, 64, 1) * (-COS_POLY[-1] * SIN_POLY[-1])
    predicted = jnp.where(lanes < 64, real, imag)
    res = jnp.where(index < total, observed[...].astype(F32) - predicted, 0.0).astype(BF16)
    residual[...] = res
    sums = lax.dot_general(weights[...], res, NT, preferred_element_type=F32)
    fields[0:1, :] = sums[0:1] + sums[1:2] + sums[2:3]
    fields[1:2, :] = sums[3:4] + sums[4:5] + sums[5:6]
    fields[2:4, :] = cells[...].astype(F32)
    fields[4:6, :] = jnp.zeros((2, rows), F32)
    fields[6:8, :] = 0.5 * fractions[...]
    everything = fields[...]
    row_of = lax.broadcasted_iota(jnp.int32, (4, slot), 0)
    place = lax.broadcasted_iota(jnp.int32, (4, slot), 1)
    for t in range(tiles):
        turned = pltpu.roll(everything, (rows - start[t]) & (rows - 1), 1)[:, :slot]
        moved = jnp.where((row_of >= 2) | (place < counts[0, t]), turned[:4], 0.0)
        halves = turned[4:]
        for owner in range(owners):
            base = float((t * owners + owner) * (GRID // (tiles * owners)))
            packed[owner, t] = (moved - jnp.where(row_of == 2, base, 0.0)) + halves


def tap_weights(position, count):
    start = jnp.floor(position)
    fraction = 2.0 * (position - start)
    first = start.astype(jnp.int32)
    lane = lax.broadcasted_iota(jnp.int32, (8, count), 0)
    tap = (lane - first) & 7
    off = (tap - 3).astype(F32) - fraction
    return jnp.exp2(off * off * -0.7213475204444817), (first + tap) >> 3


def grid_kernel(got, near, out, far, acc, sem):
    leave = pltpu.make_async_copy(near, far, sem)
    leave.start()
    sources, _, slot = got.shape
    group = 32
    count = group * slot
    width = out.shape[2]
    acc[...] = jnp.zeros(acc.shape, F32)
    lines = lax.broadcasted_iota(jnp.int32, (BAND // 8, 8, count), 0)
    columns = lax.broadcasted_iota(jnp.int32, (width // 8, 8, count), 0)

    def step(number, carry):
        data = jnp.concatenate([got[number * group + k] for k in range(group)], axis=1)
        weight, place = tap_weights(data[3:4], count)
        here = lines == place[None]
        left = jnp.concatenate(
            [
                jnp.where(here, (weight * data[k : k + 1])[None], 0.0).astype(BF16).reshape(BAND, count)
                for k in range(2)
            ]
        )
        weight, place = tap_weights(data[2:3], count)
        spread = jnp.where(columns == place[None], weight[None], 0.0).astype(BF16).reshape(width, count)
        acc[...] += lax.dot_general(left, spread, NT, preferred_element_type=F32)
        return carry

    lax.fori_loop(0, sources // group, step, 0)
    upper = lax.broadcasted_iota(jnp.int32, (8, width), 0) < 4
    for g in range(BAND // 8):
        real = acc[8 * g : 8 * g + 8]
        imag = acc[BAND + 8 * g : BAND + 8 * g + 8]
        out[2 * g] = jnp.where(upper, real, pltpu.roll(imag, 4, 0)).astype(BF16)
        out[2 * g + 1] = jnp.where(upper, pltpu.roll(real, 4, 0), imag).astype(BF16)
    leave.wait()


def sum_kernel(got, out):
    blocks, _, lines, width = got.shape
    share = lines // 2
    for b in range(blocks):
        total = jnp.sum(got[b].astype(F32), axis=0)
        for c in range(2):
            for j in range(share):
                out[j, c : c + 1, b * width : (b + 1) * width] = total[c * share + j : c * share + j + 1]


def on_device(spectra, positions, observed, cells, fractions, bucket_counts, chan_weights):
    rows = observed.shape[0]
    tiles = lax.axis_size(TILE)
    owners = lax.axis_size(VIS)
    slot = rows // 2
    width = GRID // tiles
    plane = ("vis_1", "vis_a", "tile_0")
    members = lax.axis_size(plane)
    count = spectra.shape[1]
    line = lax.axis_size(LINE)
    vmem = pl.BlockSpec(memory_space=pltpu.VMEM)
    far = pl.BlockSpec(memory_space=pltpu.HBM)
    mine, near_counts = pl.pallas_call(
        component_kernel,
        out_shape=(
            jax.ShapeDtypeStruct((members, count, 128), BF16),
            jax.ShapeDtypeStruct(bucket_counts.shape, jnp.int32),
        ),
        in_specs=[vmem] * 3,
        out_specs=(vmem,) * 2,
        name="components",
        compiler_params=LIMIT,
    )(spectra.T, positions, bucket_counts)
    own = lax.all_to_all(mine, plane, 0, 0, tiled=True).reshape(members * count, 128)
    swap = [(0, 1), (1, 0)]
    here = [own]
    next_to = lax.ppermute(own, "vis_b", swap)
    other = lax.ppermute(own, "tile_1", swap)
    sums = jax.ShapeDtypeStruct((rows, 128), F32)
    factors, cos_sum, sin_sum, weight_rows = pl.pallas_call(
        first_kernel,
        out_shape=(
            jax.ShapeDtypeStruct((rows, 128), BF16),
            sums,
            sums,
            jax.ShapeDtypeStruct((8, 128), BF16),
        ),
        in_specs=[vmem] * (len(here) + 3),
        out_specs=(vmem,) * 4,
        name="predict_first",
        compiler_params=LIMIT,
    )(*here, cells, fractions, chan_weights[None, :])
    middle = pl.pallas_call(
        middle_kernel,
        out_shape=(sums, sums),
        in_specs=[vmem] * 4,
        out_specs=(vmem, vmem),
        name="predict_middle",
        compiler_params=LIMIT,
    )
    cos_sum, sin_sum = middle(other, factors, cos_sum, sin_sum)
    next_to, cos_sum, sin_sum = lax.optimization_barrier((next_to, cos_sum, sin_sum))
    there = [lax.ppermute(next_to, "tile_1", swap)]
    cos_sum, sin_sum = middle(next_to, factors, cos_sum, sin_sum)
    near_residual, packed = pl.pallas_call(
        second_kernel,
        out_shape=(
            jax.ShapeDtypeStruct(observed.shape, BF16),
            jax.ShapeDtypeStruct((line, tiles, 4, slot), F32),
        ),
        in_specs=[pl.BlockSpec(memory_space=pltpu.SMEM)] + [vmem] * 8,
        out_specs=(vmem, vmem),
        scratch_shapes=[pltpu.VMEM((8, rows), F32)],
        name="predict_second",
        compiler_params=LIMIT,
    )(
        near_counts, *there, factors, cos_sum, sin_sum,
        cells, fractions, observed, weight_rows,
    )
    got = lax.all_to_all(
        packed.reshape(line * tiles, 4, slot), LINE + TILE, 0, 0, tiled=True
    )
    share = BAND // owners
    block = width // line
    partial, residual = pl.pallas_call(
        grid_kernel,
        out_shape=(
            jax.ShapeDtypeStruct((owners, 2 * share, block), BF16),
            jax.ShapeDtypeStruct(observed.shape, BF16),
        ),
        in_specs=[vmem] * 2,
        out_specs=(vmem, far),
        scratch_shapes=[pltpu.VMEM((2 * BAND, block), F32), pltpu.SemaphoreType.DMA],
        name="gridding",
        compiler_params=LIMIT,
    )(got, near_residual)
    parts = lax.all_to_all(partial, VIS, 0, 0, tiled=True)
    total = pl.pallas_call(
        sum_kernel,
        out_shape=jax.ShapeDtypeStruct((share, 2, width), F32),
        in_specs=[vmem],
        out_specs=vmem,
        name="add_shares",
        compiler_params=LIMIT,
    )(parts.reshape(line, owners // line, 2 * share, block))
    return residual, total


def solution(mesh):
    torus = Mesh(mesh.devices.reshape(2, 2, 8, 4, 2), VIS_TILE)
    return jax.shard_map(
        on_device,
        mesh=torus,
        in_specs=(
            P(None, VIS_TILE),
            P(None, VIS_TILE),
            P(VIS_TILE, None),
            P(None, VIS_TILE),
            P(None, VIS_TILE),
            P(VIS_TILE, None),
            P(),
        ),
        out_specs=(P(VIS_TILE, None), P(VIS, None, TILE)),
        check_vma=False,
    )
```
